512 devices in a mesh: dp: 64 (over z, y), tensor: 8 (over x, core).
Axes of the slice: x: 4, y: 4, z: 16, core: 2. Of those that a mesh axis runs over, the one named last changes fastest.
Arguments:
- layer_input: bfloat16 [8192, 8192], P('dp', 'tensor'), may hold values from -6 to 6
- output_grad: bfloat16 [8192, 8192], P('dp', 'tensor'), may hold values from -0.06591797 to 0.06591797
- gate_pre: bfloat16 [8192, 28672], P('dp', 'tensor'), may hold values from -6 to 6
- up_pre: bfloat16 [8192, 28672], P('dp', 'tensor'), may hold values from -6 to 6
- hidden_grad: bfloat16 [8192, 28672], P('dp', 'tensor'), may hold values from -0.06591797 to 0.06591797
- tile_list: int32 [448, 3], P('tensor'), may hold values from 0 to 63, as said below
- tile_slots: int32 [448], P('tensor'), may hold values from 0 to 127, as said below
- first_codes: int32 [8, 128, 16384], P('tensor', 'dp'), may hold values from 0 to 255
- second_codes: int32 [8, 128, 16384], P('tensor', 'dp'), may hold values from 0 to 255
- first_absmax: float32 [8, 128, 8], P('tensor', 'dp'), may hold values from 0.05 to 0.5
- second_absmax: float32 [8, 128, 8], P('tensor', 'dp'), may hold values from 0.005 to 0.05
- signed_map: float32 [256], replicated, may hold values from -1 to 1
- unsigned_map: float32 [256], replicated, may hold values from 0.05 to 1
Outputs:
- update_tiles: bfloat16 [448, 128, 128], P('tensor')
- first_moment: float32 [8, 128, 16384], P('tensor', 'dp')
- second_moment: float32 [8, 128, 16384], P('tensor', 'dp')
The draws below stay inside these ranges and needn't reach their ends.
Inputs may be any that keep to these rules, and one draw needn't show every extreme that they name: `tile_list`: within each group of 56 rows that belongs to one tensor index the triples are distinct; the first entry is below 64, the second below 28, the third is 0, 1 or 2. `tile_slots`: within each group of 56 entries the slots are distinct; a dp index owns slots s with s // 2 equal to it, so it holds at most 2 tiles of a group, and in every group some dp index holds exactly 2.
All inputs are finite; a program needn't handle non-finite values.
Results may differ from the reference program's by a relative error of at most 0.0085.
Values may be sent and summed in bfloat16 or wider, within the bound.
A program may use at most 64 MiB of HBM per device.

```python
import math
import jax
import jax.numpy as jnp
from jax import lax

D = 8192
FF = 28672
CAP = 2
TB = 128
QB = 2048
STEP = 10
TILES = 56
TOKENS = 8192
N_DP = 64
N_TENSOR = 8


def draw_tile_list(key, part):
    width_count = D // TB
    hidden_count = FF // (TB * N_TENSOR)
    combos = width_count * hidden_count * 3
    group_keys = jax.random.split(key, N_TENSOR)
    chosen = jax.vmap(lambda sub_key: jax.random.permutation(sub_key, combos)[:TILES])(group_keys)
    chosen = chosen.reshape(-1).astype(jnp.int32)
    width_block = chosen % width_count
    rest_part = chosen // width_count
    return jnp.stack([width_block, rest_part % hidden_count, rest_part // hidden_count], axis=1).astype(jnp.int32)


def draw_tile_slots(key, part):
    slot_count = N_DP * CAP

    def one_group(sub_key):
        first_key, second_key, third_key = jax.random.split(sub_key, 3)
        order_rank = jnp.argsort(jax.random.permutation(first_key, slot_count)).astype(jnp.int32)
        full_owner = jax.random.randint(second_key, (), 0, N_DP)
        slot_ids = jnp.arange(slot_count, dtype=jnp.int32)
        scores = order_rank + jnp.where(slot_ids // CAP == full_owner, -slot_count, 0)
        picked = jnp.argsort(scores)[:TILES].astype(jnp.int32)
        return picked[jax.random.permutation(third_key, TILES)]
    group_keys = jax.random.split(jax.random.fold_in(key, 7), N_TENSOR)
    return jax.vmap(one_group)(group_keys).reshape(-1).astype(jnp.int32)


def touch_ends(entries, stream_key, smallest, top_value):
    dims = entries.shape
    place = [jax.random.randint(jax.random.fold_in(stream_key, axis), (), 0, dims[axis]) for axis in range(len(dims))]
    entries = entries.at[tuple(place)].set(smallest)
    longest = dims.index(max(dims))
    place[longest] = (place[longest] + 1) % dims[longest]
    return entries.at[tuple(place)].set(top_value)


def steps_of(rng, dims, pieces, low, high):
    loudness, own = 1.0, jax.random.fold_in(rng, 6)
    for position, shards_of in pieces:
        draws = jnp.exp(jax.random.uniform(jax.random.fold_in(own, position), (shards_of,), jnp.float32, low / len(pieces), high / len(pieces)))
        loudness = loudness * jnp.repeat(draws, dims[position] // shards_of).reshape([-1 if axis == position else 1 for axis in range(len(dims))])
    return loudness


def scatter_about(stream_key, dims, deviation, most, pieces=(), kind=jnp.bfloat16):
    values = jax.random.normal(stream_key, dims, jnp.float32) * deviation
    if len(pieces) > 0:
        values = steps_of(stream_key, dims, pieces, -0.22, 0.18) * values
    return jnp.clip(values, min=-most, max=most).astype(kind)


def setup_inputs(seed: int = 0) -> dict:
    key_of = jax.random.split(jax.random.key(seed), 14)
    return {
        "layer_input": scatter_about(key_of[0], (TOKENS, D), 1.0, 6.0, ((0, 64), (1, 8))),
        "output_grad": scatter_about(key_of[1], (TOKENS, D), 0.011, 0.06591797, ((0, 64), (1, 8))),
        "gate_pre": scatter_about(key_of[2], (TOKENS, FF), 1.0, 6.0, ((0, 64), (1, 8))),
        "up_pre": scatter_about(key_of[3], (TOKENS, FF), 1.0, 6.0, ((0, 64), (1, 8))),
        "hidden_grad": scatter_about(key_of[4], (TOKENS, FF), 0.011, 0.06591797, ((0, 64), (1, 8))),
        "tile_list": draw_tile_list(jax.random.fold_in(key_of[13], 71), 0),
        "tile_slots": draw_tile_slots(jax.random.fold_in(key_of[13], 71), 0),
        "first_codes": touch_ends(jax.random.randint(key_of[7], (N_TENSOR, N_DP * CAP, TB * TB), 0, 256), jax.random.fold_in(key_of[7], 1), 0, 255).astype(jnp.int32),
        "second_codes": touch_ends(jax.random.randint(key_of[8], (N_TENSOR, N_DP * CAP, TB * TB), 0, 256), jax.random.fold_in(key_of[8], 1), 0, 255).astype(jnp.int32),
        "first_absmax": jnp.clip(jnp.exp(math.log(0.5) - 2.3025851 * jax.random.uniform(key_of[9], (N_TENSOR, N_DP * CAP, TB * TB // QB), jnp.float32) ** steps_of(key_of[9], (N_TENSOR, N_DP * CAP, TB * TB // QB), ((0, 8), (1, 64)), -0.2, 0.2)), 0.05, 0.5),
        "second_absmax": jnp.clip(jnp.exp(math.log(0.05) - 2.3025851 * jax.random.uniform(key_of[10], (N_TENSOR, N_DP * CAP, TB * TB // QB), jnp.float32) ** steps_of(key_of[10], (N_TENSOR, N_DP * CAP, TB * TB // QB), ((0, 8), (1, 64)), -0.2, 0.2)), 0.005, 0.05),
        "signed_map": jnp.clip(jax.random.uniform(key_of[11], (256,), jnp.float32, -1.0, 1.0), -1.0, 1.0),
        "unsigned_map": jnp.clip(jnp.exp(jax.random.uniform(key_of[12], (256,), jnp.float32, math.log(0.05), math.log(1.0))), 0.05, 1.0),
    }


BETA_FIRST = 0.9
BETA_SECOND = 0.99
EPSILON = 1e-08

def reference(layer_input, output_grad, gate_pre, up_pre, hidden_grad, tile_list, tile_slots, first_codes, second_codes, first_absmax, second_absmax, signed_map, unsigned_map):
    shard_tiles = FF // N_TENSOR // TB
    group_index = (jnp.arange(N_TENSOR * TILES, dtype=jnp.int32) // TILES).astype(jnp.int32)
    tile_rows = jnp.concatenate([tile_list, group_index[:, None]], axis=1).astype(jnp.int32)

    def one_tile(entry_row):
        width_start = (entry_row[0] * TB).astype(jnp.int32)
        hidden_start = ((entry_row[3] * shard_tiles + entry_row[1]) * TB).astype(jnp.int32)
        matrix_id = entry_row[2]
        input_block = lax.dynamic_slice_in_dim(layer_input, width_start, TB, 1)
        output_block = lax.dynamic_slice_in_dim(output_grad, width_start, TB, 1)
        gate_value = lax.dynamic_slice_in_dim(gate_pre, hidden_start, TB, 1).astype(jnp.float32)
        up_value = lax.dynamic_slice_in_dim(up_pre, hidden_start, TB, 1).astype(jnp.float32)
        grad_value = lax.dynamic_slice_in_dim(hidden_grad, hidden_start, TB, 1).astype(jnp.float32)
        sigmoid_gate = jax.nn.sigmoid(gate_value)
        silu_gate = gate_value * sigmoid_gate
        hidden = (silu_gate * up_value).astype(jnp.bfloat16)
        gate_grad = (grad_value * up_value * sigmoid_gate * (1.0 + gate_value * (1.0 - sigmoid_gate))).astype(jnp.bfloat16)
        up_grad = (grad_value * silu_gate).astype(jnp.bfloat16)
        gate_term = jnp.dot(input_block.T, gate_grad, preferred_element_type=jnp.float32)
        up_term = jnp.dot(input_block.T, up_grad, preferred_element_type=jnp.float32)
        down_term = jnp.dot(hidden.T, output_block, preferred_element_type=jnp.float32)
        return jnp.where(matrix_id == 0, gate_term, jnp.where(matrix_id == 1, up_term, down_term))
    tile_grads = lax.map(one_tile, tile_rows)
    slot_count = N_DP * CAP
    slot_grad = jnp.zeros((N_TENSOR, slot_count, TB * TB), jnp.float32)
    slot_grad = slot_grad.at[group_index, tile_slots].set(tile_grads.reshape(N_TENSOR * TILES, TB * TB))
    first_old = signed_map[first_codes] * jnp.repeat(first_absmax, QB, axis=2)
    second_old = unsigned_map[second_codes] * jnp.repeat(second_absmax, QB, axis=2)
    first_moment = BETA_FIRST * first_old + (1.0 - BETA_FIRST) * slot_grad
    second_moment = BETA_SECOND * second_old + (1.0 - BETA_SECOND) * slot_grad * slot_grad
    first_hat = first_moment / (1.0 - BETA_FIRST ** STEP)
    second_hat = second_moment / (1.0 - BETA_SECOND ** STEP)
    slot_update = (first_hat / (jnp.sqrt(second_hat) + EPSILON)).astype(jnp.bfloat16)
    update_tiles = slot_update[group_index, tile_slots].reshape(N_TENSOR * TILES, TB, TB)
    return (update_tiles, first_moment, second_moment)
```

```python
import functools

import jax
import jax.numpy as jnp
from jax import lax
from jax.experimental import pallas as pl
from jax.experimental.pallas import tpu as pltpu
from jax.sharding import PartitionSpec as P

CAP = 2
TB = 128
QB = 2048
STEP = 10
BETA_FIRST = 0.9
BETA_SECOND = 0.99
EPSILON = 1e-08

NX, NY, NZ = 4, 4, 16
TILES = 56
WB = 64
HB = 28
OWN = WB // 8
ROWS = TILES * TB // (NY * NZ)
HALF = NZ // 2
MESH = pl.DeviceIdType.MESH
F32, BF16 = jnp.float32, jnp.bfloat16


def up_to(value, size):
    return lax.rem(value, size)


class Place:
    def __init__(self):
        dp, t = lax.axis_index("dp"), lax.axis_index("tensor")
        self.dp, self.t = dp, t
        self.z, self.y = dp // NY, lax.rem(dp, NY)
        self.x, self.c = t // 2, lax.rem(t, 2)

    def along_x(self, d):
        return (self.dp, up_to(self.x + NX + d, NX) * 2 + self.c)

    def partner(self):
        return (self.dp, self.x * 2 + 1 - self.c)

    def along_y(self, d):
        return (self.z * NY + up_to(self.y + NY + d, NY), self.t)

    def along_z(self, d):
        return (up_to(self.z + NZ + d, NZ) * NY + self.y, self.t)


def remote(src, dst, send, recv, device):
    return pltpu.make_async_remote_copy(
        src_ref=src, dst_ref=dst, send_sem=send, recv_sem=recv, device_id=device, device_id_type=MESH
    )


class Gather:
    def __init__(self, place, left, right, send, recv):
        self.place, self.left, self.right, self.send, self.recv = place, left, right, send, recv
        self.sent = []

    def piece(self, d, other, p):
        pc = self.place
        core = 1 - pc.c if other else pc.c
        owner = up_to(pc.x + NX + d, NX) * 2 + core
        if p < 2:
            return self.right.at[pl.ds(2 * HB + owner * OWN + p * 4, 4)]
        return self.left.at[pl.ds(owner * OWN + (p - 2) * 4, 4)]

    def copy(self, route, p):
        pc = self.place
        shift = {0: 0, 1: 0, 2: 0, 3: -1, 4: 1, 5: -1 if p % 2 == 0 else 1, 6: 2}[route]
        to = {0: pc.along_x(1), 1: pc.along_x(-1), 5: pc.along_x(1 if p % 2 == 0 else -1)}.get(route)
        to = pc.partner() if to is None else to
        block = self.piece(shift, False, p)
        return remote(block, block, self.send.at[route, p], self.recv.at[route, p], to)

    def start(self, route, p):
        one = self.copy(route, p)
        one.start()
        self.sent.append(one)

    def arrived(self, route, p):
        shift, other = {
            0: (-1, False),
            1: (1, False),
            2: (0, True),
            3: (-1, True),
            4: (1, True),
            5: (2, False),
            6: (2, True),
        }[route]
        block = self.piece(shift, other, p)
        remote(
            block, block, self.send.at[route, p], self.recv.at[route, p], self.place.partner()
        ).wait_recv()

    def begin(self, p):
        for route in (0, 1, 2):
            self.start(route, p)

    def step(self, i):
        if i < 4:
            self.arrived(0, i)
            if i % 2 == 0:
                self.start(5, i)
            self.start(3, i)
            self.arrived(1, i)
            if i % 2 == 1:
                self.start(5, i)
            self.start(4, i)
        elif i < 8:
            self.arrived(5, i - 4)
            self.start(6, i - 4)

    def finish(self):
        for p in range(4):
            for route in (2, 3, 4, 6):
                self.arrived(route, p)
        for one in self.sent:
            one.wait_send()


class Scatter:
    def __init__(self, place, source, bufs, send, recv, kept):
        self.place, self.source, self.send, self.recv, self.kept = place, source, send, recv, kept
        self.s1, self.r1, self.s2, self.r2, self.sz, self.rz = bufs
        self.sent = []

    def own(self, zz, dy):
        yy = up_to(self.place.y + NY + dy, NY)
        start = pl.multiple_of((zz * NY + yy) * ROWS, 16)
        return self.source[:, pl.ds(start, ROWS), :]

    def zs(self, j):
        z = self.place.z
        return up_to(z + HALF - j, NZ), up_to(z + NZ - (HALF - 1 - j), NZ)

    def copy(self, kind, d, j):
        src, dst = ((self.s1, self.r1), (self.s2, self.r2), (self.sz, self.rz))[kind]
        way = 1 if d == 0 else -1
        to = self.place.along_z(way) if kind == 2 else self.place.along_y(way)
        return remote(src.at[d, j], dst.at[d, j], self.send.at[kind, d, j], self.recv.at[kind, d, j], to)

    def start(self, kind, d, j):
        one = self.copy(kind, d, j)
        one.start()
        self.sent.append(one)

    def first(self, j):
        za, zb = self.zs(j)
        self.s1[0, j] = self.own(za, 2)
        self.start(0, 0, j)
        self.s1[1, j] = self.own(zb, 2)
        self.start(0, 1, j)

    def second(self, j):
        za, zb = self.zs(j)
        self.s2[0, j, 1] = self.own(zb, 1)
        self.s2[1, j, 0] = self.own(za, -1)
        self.copy(0, 0, j).wait_recv()
        self.s2[0, j, 0] = (self.r1[0, j].astype(F32) + self.own(za, 1).astype(F32)).astype(BF16)
        self.start(1, 0, j)
        self.copy(0, 1, j).wait_recv()
        self.s2[1, j, 1] = (self.r1[1, j].astype(F32) + self.own(zb, -1).astype(F32)).astype(BF16)
        self.start(1, 1, j)

    def third(self, j):
        za, zb = self.zs(j)
        self.copy(1, 0, j).wait_recv()
        self.copy(1, 1, j).wait_recv()
        sum_a = self.own(za, 0).astype(F32) + self.r2[0, j, 0].astype(F32) + self.r2[1, j, 0].astype(F32)
        sum_b = self.own(zb, 0).astype(F32) + self.r2[0, j, 1].astype(F32) + self.r2[1, j, 1].astype(F32)
        if j > 0:
            self.copy(2, 0, j - 1).wait_recv()
            sum_a = sum_a + self.rz[0, j - 1].astype(F32)
        self.sz[0, j] = sum_a.astype(BF16)
        self.start(2, 0, j)
        if j > 0:
            self.copy(2, 1, j - 1).wait_recv()
            sum_b = sum_b + self.rz[1, j - 1].astype(F32)
        if j < HALF - 1:
            self.sz[1, j] = sum_b.astype(BF16)
            self.start(2, 1, j)
        else:
            self.kept[...] = sum_b

    def slot(self, i):
        if i < HALF:
            self.first(i)
        if 0 <= i - 1 < HALF:
            self.second(i - 1)
        if 0 <= i - 2 < HALF:
            self.third(i - 2)

    def finish(self):
        self.copy(2, 0, HALF - 1).wait_recv()
        self.kept[...] = self.kept[...] + self.rz[0, HALF - 1].astype(F32)
        for one in self.sent:
            one.wait_send()


class Spread:
    def __init__(self, place, rows, zsend, zrecv, ysend, yrecv, give):
        self.place, self.rows, self.give = place, rows, give
        self.zsend, self.zrecv, self.ysend, self.yrecv = zsend, zrecv, ysend, yrecv
        self.sent = []

    def zq(self, q):
        z = self.place.z
        if q == 0:
            return z
        if q % 2 == 1:
            return up_to(z + NZ - 1 - (q - 1) // 2, NZ)
        return up_to(z + 1 + (q - 2) // 2, NZ)

    def at(self, zz, dy):
        return zz * NY + up_to(self.place.y + NY + dy, NY)

    def zcopy(self, d, j, received):
        z = self.place.z
        back = j + 1 if received else j
        zz = up_to(z + NZ - back, NZ) if d == 0 else up_to(z + back, NZ)
        ref = self.rows.at[self.at(zz, 0)]
        to = self.place.along_z(1 if d == 0 else -1)
        return remote(ref, ref, self.zsend.at[d, j], self.zrecv.at[d, j], to)

    def ycopy(self, hop, d, q, received):
        way = 1 if d == 0 else -1
        dy = -way * (hop + 1) if received else -way * hop
        ref = self.rows.at[self.at(self.zq(q), dy)]
        if hop == 1:
            ref = ref.at[d]
        to = self.place.along_y(way)
        return remote(ref, ref, self.ysend.at[hop, d, q], self.yrecv.at[hop, d, q], to)

    def start(self, one):
        one.start()
        self.sent.append(one)

    def out_y(self, q):
        self.start(self.ycopy(0, 0, q, False))
        self.start(self.ycopy(0, 1, q, False))

    def on_y(self, q):
        self.ycopy(0, 0, q, True).wait_recv()
        self.start(self.ycopy(1, 0, q, False))
        self.ycopy(0, 1, q, True).wait_recv()
        self.start(self.ycopy(1, 1, q, False))

    def done(self, q):
        self.ycopy(1, 0, q, True).wait_recv()
        self.ycopy(1, 1, q, True).wait_recv()
        zz = self.zq(q)
        for dy in range(NY):
            self.give(self.at(zz, dy))

    def run(self):
        self.start(self.zcopy(0, 0, False))
        self.start(self.zcopy(1, 0, False))
        self.out_y(0)
        groups = [[0]]
        for j in range(HALF + 4):
            if j < HALF:
                group = [1 + 2 * j]
                self.zcopy(0, j, True).wait_recv()
                if j < HALF - 1:
                    self.start(self.zcopy(0, j + 1, False))
                    self.zcopy(1, j, True).wait_recv()
                    if j < HALF - 2:
                        self.start(self.zcopy(1, j + 1, False))
                    group.append(2 + 2 * j)
                for q in group:
                    self.out_y(q)
                groups.append(group)
            if j < len(groups):
                for q in groups[j]:
                    self.on_y(q)
            if 0 <= j - 2 < len(groups):
                for q in groups[j - 2]:
                    self.done(q)
        for one in self.sent:
            one.wait_send()


def dequantize(fscale, sscale, fcodes, scodes, smap, umap, exact, rounded):
    for a, (codes, table, scale) in enumerate(((fcodes, smap, fscale), (scodes, umap, sscale))):
        low_table = jnp.broadcast_to(table[0:1, :], (16, TB))
        high_table = jnp.broadcast_to(table[1:2, :], (16, TB))
        for s in range(CAP):
            for b in range(TB * TB // QB):
                block = slice(b * 16, (b + 1) * 16)
                code = codes[s, block, :]
                low = jnp.bitwise_and(code, TB - 1)
                value = jnp.where(
                    code < TB,
                    jnp.take_along_axis(low_table, low, axis=1, mode="promise_in_bounds"),
                    jnp.take_along_axis(high_table, low, axis=1, mode="promise_in_bounds"),
                )
                value = value * scale[s, b]
                exact[a, s, block, :] = value
                rounded[a, s, block, :] = value.astype(BF16)
        rounded[a, CAP] = jnp.zeros((TB, TB), BF16)


def kernel(
    list_ref,
    slots_ref,
    exact_ref,
    rounded_ref,
    input_ref,
    grad_ref,
    gate_ref,
    up_ref,
    hgrad_ref,
    update_ref,
    first_ref,
    second_ref,
    left,
    right,
    parts,
    states,
    rows,
    summed,
    old_kept,
    sum_kept,
    e1,
    f1,
    e2,
    f2,
    ez,
    fz,
    p1,
    q1,
    p2,
    q2,
    pz,
    qz,
    gsend,
    grecv,
    esend,
    erecv,
    psend,
    precv,
    zsend,
    zrecv,
    ysend,
    yrecv,
):
    place = Place()
    barrier = pltpu.get_barrier_semaphore()
    near = [place.partner()]
    for d in (1, -1):
        near += [place.along_x(d), place.along_y(d), place.along_z(d)]
    for device in near:
        pl.semaphore_signal(barrier, inc=1, device_id=device, device_id_type=MESH)

    gather = Gather(place, left, right, gsend, grecv)
    for j in range(OWN):
        right[2 * HB + place.t * OWN + j] = grad_ref[:, j * TB : (j + 1) * TB]
    pl.semaphore_wait(barrier, len(near))
    gather.begin(0)
    gather.begin(1)
    for j in range(OWN):
        left[place.t * OWN + j] = input_ref[:, j * TB : (j + 1) * TB].T
    gather.begin(2)
    gather.begin(3)

    def fill(k, carry):
        slot = slots_ref[k]
        mine = jnp.where(lax.shift_right_logical(slot, 1) == place.dp, jnp.bitwise_and(slot, 1), CAP)
        for a in range(2):
            states[a, pl.ds(pl.multiple_of(k * TB, TB), TB), :] = rounded_ref[a, mine]
        return carry

    lax.fori_loop(0, TILES, fill, 0)

    def activations(i):
        for h in range(4 * i, 4 * i + 4):
            cols = slice(h * TB, (h + 1) * TB)
            gate = gate_ref[:, cols].astype(F32)
            up = up_ref[:, cols].astype(F32)
            grad = hgrad_ref[:, cols].astype(F32)
            sigmoid = 1.0 / (1.0 + jnp.exp(-gate))
            silu = gate * sigmoid
            left[WB + h] = (silu * up).astype(BF16).T
            right[h] = (grad * up * sigmoid * (1.0 + gate * (1.0 - sigmoid))).astype(BF16)
            right[HB + h] = (grad * silu).astype(BF16)

    olds = Scatter(place, states, (e1, f1, e2, f2, ez, fz), esend, erecv, old_kept)
    for i in range(HALF + 2):
        olds.slot(i)
        gather.step(i)
        if i < HB // 4:
            activations(i)
    olds.finish()
    gather.finish()

    def multiply(k, carry):
        width, hidden, matrix = list_ref[k, 0], list_ref[k, 1], list_ref[k, 2]
        li = jnp.where(matrix == 2, WB + hidden, width)
        ri = jnp.where(matrix == 2, 2 * HB + width, jnp.where(matrix == 1, HB + hidden, hidden))
        tile = jnp.dot(left[li], right[ri], preferred_element_type=F32)
        parts[0, pl.ds(pl.multiple_of(k * TB, TB), TB), :] = tile.astype(BF16)
        return carry

    lax.fori_loop(0, TILES, multiply, 0, unroll=4)

    sums = Scatter(place, parts, (p1, q1, p2, q2, pz, qz), psend, precv, sum_kept)
    for i in range(HALF + 2):
        sums.slot(i)
    sums.finish()

    def moments(first_old, second_old, grad):
        first = BETA_FIRST * first_old + (1.0 - BETA_FIRST) * grad
        second = BETA_SECOND * second_old + (1.0 - BETA_SECOND) * grad * grad
        return first, second

    grad = sum_kept[0]
    first, second = moments(old_kept[0], old_kept[1], grad)
    first_hat = first / (1.0 - BETA_FIRST**STEP)
    second_hat = second / (1.0 - BETA_SECOND**STEP)
    rows[place.dp, 0] = (first_hat / (jnp.sqrt(second_hat) + EPSILON)).astype(BF16)
    rows[place.dp, 1] = grad.astype(BF16)

    def give(dp):
        where = pl.ds(pl.multiple_of(dp * ROWS, 16), ROWS)
        update_ref[where, :] = rows[dp, 0]
        summed[pl.ds(dp * (ROWS // 16), ROWS // 16)] = rows[dp, 1].reshape(ROWS // 16, 16, TB)

    summed[pl.ds(TILES * 8, 8)] = jnp.zeros((8, 16, TB), BF16)
    Spread(place, rows, zsend, zrecv, ysend, yrecv, give).run()

    for s in range(CAP):
        mine = place.dp * CAP + s
        k = lax.fori_loop(
            0, TILES, lambda i, found: jnp.where(slots_ref[i] == mine, i, found), jnp.int32(TILES)
        )
        for b in range(8):
            block = slice(b * 16, (b + 1) * 16)
            grad = summed[k * 8 + b].astype(F32)
            first, second = moments(exact_ref[0, s, block, :], exact_ref[1, s, block, :], grad)
            first_ref[s, block, :] = first
            second_ref[s, block, :] = second


def body(
    layer_input,
    output_grad,
    gate_pre,
    up_pre,
    hidden_grad,
    tile_list,
    tile_slots,
    first_codes,
    second_codes,
    first_absmax,
    second_absmax,
    signed_map,
    unsigned_map,
):
    vmem = pl.BlockSpec(memory_space=pltpu.VMEM)
    smem = pl.BlockSpec(memory_space=pltpu.SMEM)

    def scatter_shapes(n):
        one = [pltpu.VMEM((2, HALF, n, ROWS, TB), BF16)] * 2
        two = [pltpu.VMEM((2, HALF, 2, n, ROWS, TB), BF16)] * 2
        return one + two + one

    exact, rounded = pl.pallas_call(
        dequantize,
        out_shape=(
            jax.ShapeDtypeStruct((2, CAP, TB, TB), F32),
            jax.ShapeDtypeStruct((2, CAP + 1, TB, TB), BF16),
        ),
        in_specs=[smem] * 2 + [vmem] * 4,
        out_specs=[vmem] * 2,
    )(
        first_absmax[0],
        second_absmax[0],
        first_codes.reshape(CAP, TB, TB),
        second_codes.reshape(CAP, TB, TB),
        signed_map.reshape(2, TB),
        unsigned_map.reshape(2, TB),
    )
    dma = pltpu.SemaphoreType.DMA
    update, first, second = pl.pallas_call(
        kernel,
        out_shape=(
            jax.ShapeDtypeStruct((TILES * TB, TB), BF16),
            jax.ShapeDtypeStruct((CAP, TB, TB), F32),
            jax.ShapeDtypeStruct((CAP, TB, TB), F32),
        ),
        in_specs=[smem] * 2 + [vmem] * 7,
        out_specs=[vmem] * 3,
        scratch_shapes=[
            pltpu.VMEM((WB + HB, TB, TB), BF16),
            pltpu.VMEM((WB + 2 * HB, TB, TB), BF16),
            pltpu.VMEM((1, TILES * TB, TB), BF16),
            pltpu.VMEM((2, TILES * TB, TB), BF16),
            pltpu.VMEM((NY * NZ, 2, ROWS, TB), BF16),
            pltpu.VMEM(((TILES + 1) * 8, 16, TB), BF16),
            pltpu.VMEM((2, ROWS, TB), F32),
            pltpu.VMEM((1, ROWS, TB), F32),
        ]
        + scatter_shapes(2)
        + scatter_shapes(1)
        + [dma((7, 4))] * 2
        + [dma((3, 2, HALF))] * 4
        + [dma((2, HALF))] * 2
        + [dma((2, 2, NZ))] * 2,
        compiler_params=pltpu.CompilerParams(
            collective_id=0, has_side_effects=True, vmem_limit_bytes=60 * 1024 * 1024
        ),
    )(
        tile_list,
        tile_slots,
        exact,
        rounded,
        layer_input,
        output_grad,
        gate_pre,
        up_pre,
        hidden_grad,
    )
    return (
        update.reshape(TILES, TB, TB),
        first.reshape(1, CAP, TB * TB),
        second.reshape(1, CAP, TB * TB),
    )


def solution(mesh):
    in_specs = (
        P("dp", "tensor"),
        P("dp", "tensor"),
        P("dp", "tensor"),
        P("dp", "tensor"),
        P("dp", "tensor"),
        P("tensor", None),
        P("tensor"),
        P("tensor", "dp", None),
        P("tensor", "dp", None),
        P("tensor", "dp", None),
        P("tensor", "dp", None),
        P(),
        P(),
    )
    out_specs = (P("tensor", None, None), P("tensor", "dp", None), P("tensor", "dp", None))
    return jax.shard_map(body, mesh=mesh, in_specs=in_specs, out_specs=out_specs, check_vma=False)
```

```python
import functools

import jax
import jax.numpy as jnp
from jax import lax
from jax.experimental import pallas as pl
from jax.experimental.pallas import tpu as pltpu
from jax.sharding import PartitionSpec as P

CAP = 2
TB = 128
QB = 2048
STEP = 10
BETA_FIRST = 0.9
BETA_SECOND = 0.99
EPSILON = 1e-08

NX, NY, NZ = 4, 4, 16
TILES = 56
WB = 64
HB = 28
OWN = WB // 8
ROWS = TILES * TB // (NY * NZ)
HALF = NZ // 2
LAG = 2
MESH = pl.DeviceIdType.MESH
F32, BF16 = jnp.float32, jnp.bfloat16


def up_to(value, size):
    return lax.rem(value, size)


class Place:
    def __init__(self):
        dp, t = lax.axis_index("dp"), lax.axis_index("tensor")
        self.dp, self.t = dp, t
        self.z, self.y = dp // NY, lax.rem(dp, NY)
        self.x, self.c = t // 2, lax.rem(t, 2)

    def along_x(self, d):
        return (self.dp, up_to(self.x + NX + d, NX) * 2 + self.c)

    def partner(self):
        return (self.dp, self.x * 2 + 1 - self.c)

    def along_y(self, d):
        return (self.z * NY + up_to(self.y + NY + d, NY), self.t)

    def along_z(self, d):
        return (up_to(self.z + NZ + d, NZ) * NY + self.y, self.t)


def remote(src, dst, send, recv, device):
    return pltpu.make_async_remote_copy(
        src_ref=src, dst_ref=dst, send_sem=send, recv_sem=recv, device_id=device, device_id_type=MESH
    )


class Gather:
    def __init__(self, place, left, right, send, recv):
        self.place, self.left, self.right, self.send, self.recv = place, left, right, send, recv
        self.sent = []

    def piece(self, d, other, p):
        pc = self.place
        core = 1 - pc.c if other else pc.c
        owner = up_to(pc.x + NX + d, NX) * 2 + core
        if p < 2:
            return self.right.at[pl.ds(2 * HB + owner * OWN + p * 4, 4)]
        return self.left.at[pl.ds(owner * OWN + (p - 2) * 4, 4)]

    def copy(self, route, p):
        pc = self.place
        shift = {0: 0, 1: 0, 2: 0, 3: -1, 4: 1, 5: -1 if p % 2 == 0 else 1, 6: 2}[route]
        to = {0: pc.along_x(1), 1: pc.along_x(-1), 5: pc.along_x(1 if p % 2 == 0 else -1)}.get(route)
        to = pc.partner() if to is None else to
        block = self.piece(shift, False, p)
        return remote(block, block, self.send.at[route, p], self.recv.at[route, p], to)

    def start(self, route, p):
        one = self.copy(route, p)
        one.start()
        self.sent.append(one)

    def arrived(self, route, p):
        shift, other = {
            0: (-1, False),
            1: (1, False),
            2: (0, True),
            3: (-1, True),
            4: (1, True),
            5: (2, False),
            6: (2, True),
        }[route]
        block = self.piece(shift, other, p)
        remote(
            block, block, self.send.at[route, p], self.recv.at[route, p], self.place.partner()
        ).wait_recv()

    def begin(self, p):
        for route in (0, 1, 2):
            self.start(route, p)

    def step(self, i):
        if i < 4:
            self.arrived(0, i)
            if i % 2 == 0:
                self.start(5, i)
            self.start(3, i)
            self.arrived(1, i)
            if i % 2 == 1:
                self.start(5, i)
            self.start(4, i)
        elif i < 8:
            self.arrived(5, i - 4)
            self.start(6, i - 4)

    def finish(self):
        for p in range(4):
            for route in (2, 3, 4, 6):
                self.arrived(route, p)
        for one in self.sent:
            one.wait_send()


class Scatter:
    def __init__(self, place, source, bufs, send, recv, kept):
        self.place, self.source, self.send, self.recv, self.kept = place, source, send, recv, kept
        self.s1, self.r1, self.s2, self.r2, self.sz, self.rz = bufs
        self.sent = []

    def own(self, zz, dy):
        yy = up_to(self.place.y + NY + dy, NY)
        start = pl.multiple_of((zz * NY + yy) * ROWS, 16)
        return self.source[:, pl.ds(start, ROWS), :]

    def zs(self, j):
        z = self.place.z
        return up_to(z + HALF - j, NZ), up_to(z + NZ - (HALF - 1 - j), NZ)

    def copy(self, kind, d, j):
        src, dst = ((self.s1, self.r1), (self.s2, self.r2), (self.sz, self.rz))[kind]
        way = 1 if d == 0 else -1
        to = self.place.along_z(way) if kind == 2 else self.place.along_y(way)
        return remote(src.at[d, j], dst.at[d, j], self.send.at[kind, d, j], self.recv.at[kind, d, j], to)

    def start(self, kind, d, j):
        one = self.copy(kind, d, j)
        one.start()
        self.sent.append(one)

    def first(self, j):
        za, zb = self.zs(j)
        self.s1[0, j] = self.own(za, 2)
        self.start(0, 0, j)
        self.s1[1, j] = self.own(zb, 2)
        self.start(0, 1, j)

    def second(self, j):
        za, zb = self.zs(j)
        self.s2[0, j, 1] = self.own(zb, 1)
        self.s2[1, j, 0] = self.own(za, -1)
        self.copy(0, 0, j).wait_recv()
        self.s2[0, j, 0] = (self.r1[0, j].astype(F32) + self.own(za, 1).astype(F32)).astype(BF16)
        self.start(1, 0, j)
        self.copy(0, 1, j).wait_recv()
        self.s2[1, j, 1] = (self.r1[1, j].astype(F32) + self.own(zb, -1).astype(F32)).astype(BF16)
        self.start(1, 1, j)

    def third(self, j):
        za, zb = self.zs(j)
        self.copy(1, 0, j).wait_recv()
        self.copy(1, 1, j).wait_recv()
        sum_a = self.own(za, 0).astype(F32) + self.r2[0, j, 0].astype(F32) + self.r2[1, j, 0].astype(F32)
        sum_b = self.own(zb, 0).astype(F32) + self.r2[0, j, 1].astype(F32) + self.r2[1, j, 1].astype(F32)
        if j > 0:
            self.copy(2, 0, j - 1).wait_recv()
            sum_a = sum_a + self.rz[0, j - 1].astype(F32)
        self.sz[0, j] = sum_a.astype(BF16)
        self.start(2, 0, j)
        if j > 0:
            self.copy(2, 1, j - 1).wait_recv()
            sum_b = sum_b + self.rz[1, j - 1].astype(F32)
        if j < HALF - 1:
            self.sz[1, j] = sum_b.astype(BF16)
            self.start(2, 1, j)
        else:
            self.kept[...] = sum_b

    def slot(self, i):
        if i < HALF:
            self.first(i)
        if 0 <= i - LAG < HALF:
            self.second(i - LAG)
        if 0 <= i - 2 * LAG < HALF:
            self.third(i - 2 * LAG)

    def finish(self):
        self.copy(2, 0, HALF - 1).wait_recv()
        self.kept[...] = self.kept[...] + self.rz[0, HALF - 1].astype(F32)
        for one in self.sent:
            one.wait_send()


class Pool:
    def __init__(self, place, pool, send, recv):
        self.place, self.pool, self.send, self.recv = place, pool, send, recv
        self.sent = []

    def copy(self, hop, d, received):
        way = 1 if d == 0 else -1
        back = -way * (hop + 1) if received else -way * hop
        yy = up_to(self.place.y + NY + back, NY)
        ref = self.pool.at[pl.ds(yy * CAP, CAP)] if hop == 0 else self.pool.at[yy * CAP + d]
        return remote(ref, ref, self.send.at[hop, d], self.recv.at[hop, d], self.place.along_y(way))

    def start(self, hop):
        for d in range(2):
            if hop == 1:
                self.copy(0, d, True).wait_recv()
            one = self.copy(hop, d, False)
            one.start()
            self.sent.append(one)

    def finish(self):
        for d in range(2):
            self.copy(1, d, True).wait_recv()
        for one in self.sent:
            one.wait_send()


class Olds:
    def __init__(self, place, states, out, into, send, recv, kept):
        self.place, self.states, self.out, self.into = place, states, out, into
        self.send, self.recv, self.kept = send, recv, kept
        self.sent = []

    def copy(self, d, j):
        to = self.place.along_z(1 if d == 0 else -1)
        return remote(self.out.at[d, j], self.into.at[d, j], self.send.at[d, j], self.recv.at[d, j], to)

    def own(self, zz):
        start = pl.multiple_of((zz * NY + self.place.y) * ROWS, 16)
        return self.states[:, pl.ds(start, ROWS), :].astype(F32)

    def slot(self, j):
        z = self.place.z
        far = (up_to(z + HALF - j, NZ), up_to(z + NZ - (HALF - 1 - j), NZ))
        for d in range(2):
            value = self.own(far[d])
            if j > 0:
                self.copy(d, j - 1).wait_recv()
                value = value + self.into[d, j - 1].astype(F32)
            if d == 1 and j == HALF - 1:
                self.kept[...] = value
            else:
                self.out[d, j] = value.astype(BF16)
                one = self.copy(d, j)
                one.start()
                self.sent.append(one)

    def finish(self):
        self.copy(0, HALF - 1).wait_recv()
        self.kept[...] = self.kept[...] + self.into[0, HALF - 1].astype(F32)
        for one in self.sent:
            one.wait_send()


class Spread:
    def __init__(self, place, rows, zsend, zrecv, ysend, yrecv, give, take):
        self.place, self.rows, self.give, self.take = place, rows, give, take
        self.zsend, self.zrecv, self.ysend, self.yrecv = zsend, zrecv, ysend, yrecv
        self.sent = []

    def zq(self, q):
        z = self.place.z
        if q == 0:
            return z
        if q % 2 == 1:
            return up_to(z + NZ - 1 - (q - 1) // 2, NZ)
        return up_to(z + 1 + (q - 2) // 2, NZ)

    def at(self, zz, dy):
        return zz * NY + up_to(self.place.y + NY + dy, NY)

    def zcopy(self, what, d, j, received):
        z = self.place.z
        back = j + 1 if received else j
        zz = up_to(z + NZ - back, NZ) if d == 0 else up_to(z + back, NZ)
        ref = self.rows.at[self.at(zz, 0), what]
        to = self.place.along_z(1 if d == 0 else -1)
        return remote(ref, ref, self.zsend.at[what, d, j], self.zrecv.at[what, d, j], to)

    def ycopy(self, hop, d, q, received):
        way = 1 if d == 0 else -1
        dy = -way * (hop + 1) if received else -way * hop
        ref = self.rows.at[self.at(self.zq(q), dy), 0]
        if hop == 1:
            ref = ref.at[pl.ds(0, 64)] if d == 0 else ref.at[pl.ds(64, ROWS - 64)]
        to = self.place.along_y(way)
        return remote(ref, ref, self.ysend.at[hop, d, q], self.yrecv.at[hop, d, q], to)

    def start(self, one):
        one.start()
        self.sent.append(one)

    def out_y(self, q):
        self.start(self.ycopy(0, 0, q, False))
        self.start(self.ycopy(0, 1, q, False))

    def on_y(self, q):
        self.ycopy(0, 0, q, True).wait_recv()
        self.start(self.ycopy(1, 0, q, False))
        self.ycopy(0, 1, q, True).wait_recv()
        self.start(self.ycopy(1, 1, q, False))

    def done(self, q):
        self.ycopy(1, 0, q, True).wait_recv()
        self.ycopy(1, 1, q, True).wait_recv()
        zz = self.zq(q)
        for dy in range(NY):
            self.give(self.at(zz, dy))

    def hops(self, j):
        return (0, 1) if j < HALF - 1 else (0,)

    def along_z(self, what, j):
        for d in self.hops(j):
            self.zcopy(what, d, j, True).wait_recv()
            if d in self.hops(j + 1) and j + 1 < HALF:
                self.start(self.zcopy(what, d, j + 1, False))
        return [1 + 2 * j + d for d in self.hops(j)]

    def begin(self, what):
        for d in range(2):
            self.start(self.zcopy(what, d, 0, False))

    def run(self, collect):
        self.begin(0)
        self.begin(1)
        self.out_y(0)
        self.take(self.at(self.place.z, 0))
        groups = [[0]]
        for j in range(HALF + 4):
            if j < HALF:
                group = self.along_z(0, j)
                for q in group:
                    self.out_y(q)
                groups.append(group)
            if 0 < j <= HALF:
                for q in self.along_z(1, j - 1):
                    self.take(self.at(self.zq(q), 0))
            if j == HALF:
                collect.first()
            if j < len(groups):
                for q in groups[j]:
                    self.on_y(q)
            if j == HALF + 1:
                collect.second()
            if 0 <= j - 2 < len(groups):
                for q in groups[j - 2]:
                    self.done(q)
        for one in self.sent:
            one.wait_send()


class Collect:
    def __init__(self, place, tiles, summed, out, into, relay, last, send, recv):
        self.place, self.tiles, self.summed = place, tiles, summed
        self.out, self.into, self.relay, self.last = out, into, relay, last
        self.send, self.recv = send, recv
        self.sent = []

    def copy(self, hop, d):
        src, dst = (
            (self.out.at[d], self.into.at[d]),
            (self.out.at[2, d], self.relay.at[d]),
            (self.relay.at[d], self.last.at[d]),
        )[hop]
        to = self.place.along_y(1 if d == 0 else -1)
        return remote(src, dst, self.send.at[hop, d], self.recv.at[hop, d], to)

    def start(self, hop, d):
        one = self.copy(hop, d)
        one.start()
        self.sent.append(one)

    def first(self):
        for n in (2, 0, 1):
            for s in range(CAP):
                k = self.tiles[n * CAP + s]
                for b in range(8):
                    self.out[n, s, b * 16 : (b + 1) * 16, :] = self.summed[k * 8 + b]
            if n == 2:
                self.start(1, 0)
                self.start(1, 1)
            else:
                self.start(0, n)

    def second(self):
        for d in range(2):
            self.copy(1, d).wait_recv()
            self.start(2, d)

    def finish(self):
        for hop in (0, 2):
            for d in range(2):
                self.copy(hop, d).wait_recv()
        for one in self.sent:
            one.wait_send()

    def grad(self, s, b):
        block = slice(b * 16, (b + 1) * 16)
        value = self.summed[self.tiles[3 * CAP + s] * 8 + b].astype(F32)
        for other in (self.into[0, s, block, :], self.into[1, s, block, :], self.last[s, block, :]):
            value = value + other.astype(F32)
        return value


def dequantize(fscale, sscale, fcodes, scodes, smap, umap, exact, rounded):
    for a, (codes, table, scale) in enumerate(((fcodes, smap, fscale), (scodes, umap, sscale))):
        low_table = jnp.broadcast_to(table[0:1, :], (16, TB))
        high_table = jnp.broadcast_to(table[1:2, :], (16, TB))
        for s in range(CAP):
            for b in range(TB * TB // QB):
                block = slice(b * 16, (b + 1) * 16)
                code = codes[s, block, :]
                low = jnp.bitwise_and(code, TB - 1)
                value = jnp.where(
                    code < TB,
                    jnp.take_along_axis(low_table, low, axis=1, mode="promise_in_bounds"),
                    jnp.take_along_axis(high_table, low, axis=1, mode="promise_in_bounds"),
                )
                value = value * scale[s, b]
                exact[a, s, block, :] = value
                rounded[s, a, block, :] = value.astype(BF16)


def kernel(
    list_ref,
    slots_ref,
    exact_ref,
    rounded_ref,
    input_ref,
    grad_ref,
    gate_ref,
    up_ref,
    hgrad_ref,
    update_ref,
    first_ref,
    second_ref,
    left,
    right,
    parts,
    states,
    pool,
    rows,
    summed,
    old_kept,
    sum_kept,
    oz,
    iz,
    p1,
    q1,
    p2,
    q2,
    pz,
    qz,
    cout,
    cinto,
    crelay,
    clast,
    gsend,
    grecv,
    osend,
    orecv,
    esend,
    erecv,
    psend,
    precv,
    zsend,
    zrecv,
    ysend,
    yrecv,
    csend,
    crecv,
):
    place = Place()
    barrier = pltpu.get_barrier_semaphore()
    near = [place.partner()]
    for d in (1, -1):
        near += [place.along_x(d), place.along_y(d), place.along_z(d)]
    for device in near:
        pl.semaphore_signal(barrier, inc=1, device_id=device, device_id_type=MESH)

    shared = Pool(place, pool, osend, orecv)
    pool[pl.ds(place.y * CAP, CAP)] = rounded_ref[...]
    pool[NY * CAP] = jnp.zeros((2, TB, TB), BF16)
    gather = Gather(place, left, right, gsend, grecv)
    for j in range(OWN):
        right[2 * HB + place.t * OWN + j] = grad_ref[:, j * TB : (j + 1) * TB]
    pl.semaphore_wait(barrier, len(near))
    shared.start(0)
    gather.begin(0)
    gather.begin(1)
    for j in range(OWN):
        left[place.t * OWN + j] = input_ref[:, j * TB : (j + 1) * TB].T
    gather.begin(2)
    gather.begin(3)

    def activations(i):
        for h in range(4 * i, 4 * i + 4):
            cols = slice(h * TB, (h + 1) * TB)
            gate = gate_ref[:, cols].astype(F32)
            up = up_ref[:, cols].astype(F32)
            grad = hgrad_ref[:, cols].astype(F32)
            sigmoid = 1.0 / (1.0 + jnp.exp(-gate))
            silu = gate * sigmoid
            left[WB + h] = (silu * up).astype(BF16).T
            right[h] = (grad * up * sigmoid * (1.0 + gate * (1.0 - sigmoid))).astype(BF16)
            right[HB + h] = (grad * silu).astype(BF16)

    def fill(k, carry):
        slot = slots_ref[k]
        near = lax.shift_right_logical(slot, 3) == place.z
        mine = jnp.where(near, jnp.bitwise_and(slot, NY * CAP - 1), NY * CAP)
        for a in range(2):
            states[a, pl.ds(pl.multiple_of(k * TB, TB), TB), :] = pool[mine, a]
        return carry

    olds = Olds(place, states, oz, iz, esend, erecv, old_kept)
    activations(0)
    shared.start(1)
    activations(1)
    gather.step(0)
    shared.finish()
    lax.fori_loop(0, TILES, fill, 0)
    for i in range(HALF):
        olds.slot(i)
        gather.step(i + 1)
        if i + 2 < HB // 4:
            activations(i + 2)

    def find(k, found):
        slot = slots_ref[k]
        return tuple(jnp.where(slot == one, k, old) for one, old in zip(wanted, found))

    wanted = [
        (place.z * NY + up_to(place.y + NY + dy, NY)) * CAP + s for dy in (1, -1, 2, 0) for s in range(CAP)
    ]
    tiles = lax.fori_loop(0, TILES, find, (jnp.int32(TILES),) * len(wanted))
    summed[...] = jnp.zeros(summed.shape, BF16)
    olds.finish()
    gather.finish()

    def multiply(k, carry):
        width, hidden, matrix = list_ref[0, k], list_ref[1, k], list_ref[2, k]
        li = jnp.where(matrix == 2, WB + hidden, width)
        ri = jnp.where(matrix == 2, 2 * HB + width, jnp.where(matrix == 1, HB + hidden, hidden))
        tile = jnp.dot(left[li], right[ri], preferred_element_type=F32)
        parts[0, pl.ds(pl.multiple_of(k * TB, TB), TB), :] = tile.astype(BF16)
        return carry

    lax.fori_loop(0, TILES, multiply, 0, unroll=4)

    sums = Scatter(place, parts, (p1, q1, p2, q2, pz, qz), psend, precv, sum_kept)
    for i in range(HALF + 2 * LAG):
        sums.slot(i)
    sums.finish()

    def moments(first_old, second_old, grad):
        first = BETA_FIRST * first_old + (1.0 - BETA_FIRST) * grad
        second = BETA_SECOND * second_old + (1.0 - BETA_SECOND) * grad * grad
        return first, second

    grad = sum_kept[0]
    first, second = moments(old_kept[0], old_kept[1], grad)
    first_hat = first / (1.0 - BETA_FIRST**STEP)
    second_hat = second / (1.0 - BETA_SECOND**STEP)
    rows[place.dp, 0] = (first_hat / (jnp.sqrt(second_hat) + EPSILON)).astype(BF16)
    rows[place.dp, 1] = grad.astype(BF16)

    def give(dp):
        update_ref[pl.ds(pl.multiple_of(dp * ROWS, 16), ROWS), :] = rows[dp, 0]

    def take(dp):
        summed[pl.ds(dp * (ROWS // 16), ROWS // 16)] = rows[dp, 1].reshape(ROWS // 16, 16, TB)

    collect = Collect(place, tiles, summed, cout, cinto, crelay, clast, csend, crecv)
    Spread(place, rows, zsend, zrecv, ysend, yrecv, give, take).run(collect)
    collect.finish()
    for s in range(CAP):
        for b in range(8):
            block = slice(b * 16, (b + 1) * 16)
            grad = collect.grad(s, b)
            first, second = moments(exact_ref[0, s, block, :], exact_ref[1, s, block, :], grad)
            first_ref[s, block, :] = first
            second_ref[s, block, :] = second


def body(
    layer_input,
    output_grad,
    gate_pre,
    up_pre,
    hidden_grad,
    tile_list,
    tile_slots,
    first_codes,
    second_codes,
    first_absmax,
    second_absmax,
    signed_map,
    unsigned_map,
):
    vmem = pl.BlockSpec(memory_space=pltpu.VMEM)
    smem = pl.BlockSpec(memory_space=pltpu.SMEM)

    def scatter_shapes(n):
        one = [pltpu.VMEM((2, HALF, n, ROWS, TB), BF16)] * 2
        two = [pltpu.VMEM((2, HALF, 2, n, ROWS, TB), BF16)] * 2
        return one + two + one

    exact, rounded = pl.pallas_call(
        dequantize,
        out_shape=(
            jax.ShapeDtypeStruct((2, CAP, TB, TB), F32),
            jax.ShapeDtypeStruct((CAP, 2, TB, TB), BF16),
        ),
        in_specs=[smem] * 2 + [vmem] * 4,
        out_specs=[vmem] * 2,
    )(
        first_absmax[0],
        second_absmax[0],
        first_codes.reshape(CAP, TB, TB),
        second_codes.reshape(CAP, TB, TB),
        signed_map.reshape(2, TB),
        unsigned_map.reshape(2, TB),
    )
    dma = pltpu.SemaphoreType.DMA
    update, first, second = pl.pallas_call(
        kernel,
        out_shape=(
            jax.ShapeDtypeStruct((TILES * TB, TB), BF16),
            jax.ShapeDtypeStruct((CAP, TB, TB), F32),
            jax.ShapeDtypeStruct((CAP, TB, TB), F32),
        ),
        in_specs=[smem] * 2 + [vmem] * 7,
        out_specs=[vmem] * 3,
        scratch_shapes=[
            pltpu.VMEM((WB + HB, TB, TB), BF16),
            pltpu.VMEM((WB + 2 * HB, TB, TB), BF16),
            pltpu.VMEM((1, TILES * TB, TB), BF16),
            pltpu.VMEM((2, TILES * TB, TB), BF16),
            pltpu.VMEM((NY * CAP + 1, 2, TB, TB), BF16),
            pltpu.VMEM((NY * NZ, 2, ROWS, TB), BF16),
            pltpu.VMEM(((TILES + 1) * 8, 16, TB), BF16),
            pltpu.VMEM((2, ROWS, TB), F32),
            pltpu.VMEM((1, ROWS, TB), F32),
        ]
        + [pltpu.VMEM((2, HALF, 2, ROWS, TB), BF16)] * 2
        + scatter_shapes(1)
        + [
            pltpu.VMEM((3, CAP, TB, TB), BF16),
            pltpu.VMEM((2, CAP, TB, TB), BF16),
            pltpu.VMEM((2, TB, TB), BF16),
            pltpu.VMEM((2, TB, TB), BF16),
        ]
        + [dma((7, 4))] * 2
        + [dma((2, 2))] * 2
        + [dma((2, HALF))] * 2
        + [dma((3, 2, HALF))] * 2
        + [dma((2, 2, HALF))] * 2
        + [dma((2, 2, NZ))] * 2
        + [dma((3, 2))] * 2,
        compiler_params=pltpu.CompilerParams(
            collective_id=0, has_side_effects=True, vmem_limit_bytes=60 * 1024 * 1024
        ),
    )(
        tile_list.T,
        tile_slots,
        exact,
        rounded,
        layer_input,
        output_grad,
        gate_pre,
        up_pre,
        hidden_grad,
    )
    return (
        update.reshape(TILES, TB, TB),
        first.reshape(1, CAP, TB * TB),
        second.reshape(1, CAP, TB * TB),
    )


def solution(mesh):
    in_specs = (
        P("dp", "tensor"),
        P("dp", "tensor"),
        P("dp", "tensor"),
        P("dp", "tensor"),
        P("dp", "tensor"),
        P("tensor", None),
        P("tensor"),
        P("tensor", "dp", None),
        P("tensor", "dp", None),
        P("tensor", "dp", None),
        P("tensor", "dp", None),
        P(),
        P(),
    )
    out_specs = (P("tensor", None, None), P("tensor", "dp", None), P("tensor", "dp", None))
    return jax.shard_map(body, mesh=mesh, in_specs=in_specs, out_specs=out_specs, check_vma=False)
```

```python
import functools

import jax
import jax.numpy as jnp
from jax import lax
from jax.experimental import pallas as pl
from jax.experimental.pallas import tpu as pltpu
from jax.sharding import PartitionSpec as P

CAP = 2
TB = 128
QB = 2048
STEP = 10
BETA_FIRST = 0.9
BETA_SECOND = 0.99
EPSILON = 1e-08

NX, NY, NZ = 4, 4, 16
TILES = 56
WB = 64
HB = 28
OWN = WB // 8
ROWS = TILES * TB // (NY * NZ)
HALF = NZ // 2
LAG = 2
MESH = pl.DeviceIdType.MESH
F32, BF16 = jnp.float32, jnp.bfloat16


def up_to(value, size):
    return lax.rem(value, size)


class Place:
    def __init__(self):
        dp, t = lax.axis_index("dp"), lax.axis_index("tensor")
        self.dp, self.t = dp, t
        self.z, self.y = dp // NY, lax.rem(dp, NY)
        self.x, self.c = t // 2, lax.rem(t, 2)

    def along_x(self, d):
        return (self.dp, up_to(self.x + NX + d, NX) * 2 + self.c)

    def partner(self):
        return (self.dp, self.x * 2 + 1 - self.c)

    def along_y(self, d):
        return (self.z * NY + up_to(self.y + NY + d, NY), self.t)

    def along_z(self, d):
        return (up_to(self.z + NZ + d, NZ) * NY + self.y, self.t)


def remote(src, dst, send, recv, device):
    return pltpu.make_async_remote_copy(
        src_ref=src, dst_ref=dst, send_sem=send, recv_sem=recv, device_id=device, device_id_type=MESH
    )


def leap(d, j):
    return min(2, HALF - d - j)


class Gather:
    def __init__(self, place, left, right, send, recv):
        self.place, self.left, self.right, self.send, self.recv = place, left, right, send, recv
        self.sent = []

    def piece(self, d, other, p):
        pc = self.place
        core = 1 - pc.c if other else pc.c
        owner = up_to(pc.x + NX + d, NX) * 2 + core
        if p < 2:
            return self.right.at[pl.ds(2 * HB + owner * OWN + p * 4, 4)]
        return self.left.at[pl.ds(owner * OWN + (p - 2) * 4, 4)]

    def copy(self, route, p):
        pc = self.place
        shift = {0: 0, 1: 0, 2: 0, 3: -1, 4: 1, 5: -1 if p % 2 == 0 else 1, 6: 2}[route]
        to = {0: pc.along_x(1), 1: pc.along_x(-1), 5: pc.along_x(1 if p % 2 == 0 else -1)}.get(route)
        to = pc.partner() if to is None else to
        block = self.piece(shift, False, p)
        return remote(block, block, self.send.at[route, p], self.recv.at[route, p], to)

    def start(self, route, p):
        one = self.copy(route, p)
        one.start()
        self.sent.append(one)

    def arrived(self, route, p):
        shift, other = {
            0: (-1, False),
            1: (1, False),
            2: (0, True),
            3: (-1, True),
            4: (1, True),
            5: (2, False),
            6: (2, True),
        }[route]
        block = self.piece(shift, other, p)
        remote(
            block, block, self.send.at[route, p], self.recv.at[route, p], self.place.partner()
        ).wait_recv()

    def begin(self, p):
        for route in (0, 1, 2):
            self.start(route, p)

    def step(self, i):
        if i < 4:
            self.arrived(0, i)
            if i % 2 == 0:
                self.start(5, i)
            self.start(3, i)
            self.arrived(1, i)
            if i % 2 == 1:
                self.start(5, i)
            self.start(4, i)
        elif i < 8:
            self.arrived(5, i - 4)
            self.start(6, i - 4)

    def finish(self):
        for p in range(4):
            for route in (2, 3, 4, 6):
                self.arrived(route, p)
        for one in self.sent:
            one.wait_send()


class Scatter:
    def __init__(self, place, source, bufs, send, recv, kept):
        self.place, self.source, self.send, self.recv, self.kept = place, source, send, recv, kept
        self.s1, self.r1, self.s2, self.r2, self.sz, self.rz = bufs
        self.sent = []

    def own(self, zz, dy):
        yy = up_to(self.place.y + NY + dy, NY)
        start = pl.multiple_of((zz * NY + yy) * ROWS, 16)
        return self.source[:, pl.ds(start, ROWS), :]

    def zs(self, j):
        z = self.place.z
        return up_to(z + HALF - j, NZ), up_to(z + NZ - (HALF - 1 - j), NZ)

    def copy(self, kind, d, j):
        src, dst = ((self.s1, self.r1), (self.s2, self.r2), (self.sz, self.rz))[kind]
        way = 1 if d == 0 else -1
        to = self.place.along_z(way * leap(d, j)) if kind == 2 else self.place.along_y(way)
        return remote(src.at[d, j], dst.at[d, j], self.send.at[kind, d, j], self.recv.at[kind, d, j], to)

    def start(self, kind, d, j):
        one = self.copy(kind, d, j)
        one.start()
        self.sent.append(one)

    def first(self, j):
        za, zb = self.zs(j)
        self.s1[0, j] = self.own(za, 2)
        self.start(0, 0, j)
        self.s1[1, j] = self.own(zb, 2)
        self.start(0, 1, j)

    def second(self, j):
        za, zb = self.zs(j)
        self.s2[0, j, 1] = self.own(zb, 1)
        self.s2[1, j, 0] = self.own(za, -1)
        self.copy(0, 0, j).wait_recv()
        self.s2[0, j, 0] = (self.r1[0, j].astype(F32) + self.own(za, 1).astype(F32)).astype(BF16)
        self.start(1, 0, j)
        self.copy(0, 1, j).wait_recv()
        self.s2[1, j, 1] = (self.r1[1, j].astype(F32) + self.own(zb, -1).astype(F32)).astype(BF16)
        self.start(1, 1, j)

    def third(self, j):
        za, zb = self.zs(j)
        self.copy(1, 0, j).wait_recv()
        self.copy(1, 1, j).wait_recv()
        sum_a = self.own(za, 0).astype(F32) + self.r2[0, j, 0].astype(F32) + self.r2[1, j, 0].astype(F32)
        sum_b = self.own(zb, 0).astype(F32) + self.r2[0, j, 1].astype(F32) + self.r2[1, j, 1].astype(F32)
        if j > 1:
            self.copy(2, 0, j - 2).wait_recv()
            sum_a = sum_a + self.rz[0, j - 2].astype(F32)
        self.sz[0, j] = sum_a.astype(BF16)
        self.start(2, 0, j)
        if j > 1:
            self.copy(2, 1, j - 2).wait_recv()
            sum_b = sum_b + self.rz[1, j - 2].astype(F32)
        if j < HALF - 1:
            self.sz[1, j] = sum_b.astype(BF16)
            self.start(2, 1, j)
        else:
            self.kept[...] = sum_b

    def slot(self, i):
        if i < HALF:
            self.first(i)
        if 0 <= i - LAG < HALF:
            self.second(i - LAG)
        if 0 <= i - 2 * LAG < HALF:
            self.third(i - 2 * LAG)

    def finish(self):
        for d, j in ((0, HALF - 2), (1, HALF - 2), (0, HALF - 1)):
            self.copy(2, d, j).wait_recv()
            self.kept[...] = self.kept[...] + self.rz[d, j].astype(F32)
        for one in self.sent:
            one.wait_send()


class Pool:
    def __init__(self, place, pool, send, recv):
        self.place, self.pool, self.send, self.recv = place, pool, send, recv
        self.sent = []

    def copy(self, hop, d, received):
        way = 1 if d == 0 else -1
        back = -way * (hop + 1) if received else -way * hop
        yy = up_to(self.place.y + NY + back, NY)
        ref = self.pool.at[pl.ds(yy * CAP, CAP)] if hop == 0 else self.pool.at[yy * CAP + d]
        return remote(ref, ref, self.send.at[hop, d], self.recv.at[hop, d], self.place.along_y(way))

    def start(self, hop):
        for d in range(2):
            if hop == 1:
                self.copy(0, d, True).wait_recv()
            one = self.copy(hop, d, False)
            one.start()
            self.sent.append(one)

    def finish(self):
        for d in range(2):
            self.copy(1, d, True).wait_recv()
        for one in self.sent:
            one.wait_send()


class Olds:
    def __init__(self, place, states, out, into, send, recv, kept):
        self.place, self.states, self.out, self.into = place, states, out, into
        self.send, self.recv, self.kept = send, recv, kept
        self.sent = []

    def copy(self, d, j):
        to = self.place.along_z(leap(d, j) if d == 0 else -leap(d, j))
        return remote(self.out.at[d, j], self.into.at[d, j], self.send.at[d, j], self.recv.at[d, j], to)

    def own(self, zz):
        start = pl.multiple_of((zz * NY + self.place.y) * ROWS, 16)
        return self.states[:, pl.ds(start, ROWS), :].astype(F32)

    def slot(self, j):
        z = self.place.z
        far = (up_to(z + HALF - j, NZ), up_to(z + NZ - (HALF - 1 - j), NZ))
        for d in range(2):
            value = self.own(far[d])
            if j > 1:
                self.copy(d, j - 2).wait_recv()
                value = value + self.into[d, j - 2].astype(F32)
            if d == 1 and j == HALF - 1:
                self.kept[...] = value
            else:
                self.out[d, j] = value.astype(BF16)
                one = self.copy(d, j)
                one.start()
                self.sent.append(one)

    def finish(self):
        for d, j in ((0, HALF - 2), (1, HALF - 2), (0, HALF - 1)):
            self.copy(d, j).wait_recv()
            self.kept[...] = self.kept[...] + self.into[d, j].astype(F32)
        for one in self.sent:
            one.wait_send()


class Spread:
    def __init__(self, place, rows, zsend, zrecv, ysend, yrecv, give, take):
        self.place, self.rows, self.give, self.take = place, rows, give, take
        self.zsend, self.zrecv, self.ysend, self.yrecv = zsend, zrecv, ysend, yrecv
        self.sent = []

    def zq(self, q):
        z = self.place.z
        if q == 0:
            return z
        if q % 2 == 1:
            return up_to(z + NZ - 1 - (q - 1) // 2, NZ)
        return up_to(z + 1 + (q - 2) // 2, NZ)

    def at(self, zz, dy):
        return zz * NY + up_to(self.place.y + NY + dy, NY)

    def zcopy(self, what, d, j, received):
        z = self.place.z
        step = min(2, j + 1)
        back = j + 1 if received else j + 1 - step
        zz = up_to(z + NZ - back, NZ) if d == 0 else up_to(z + back, NZ)
        ref = self.rows.at[self.at(zz, 0), what]
        to = self.place.along_z(step if d == 0 else -step)
        return remote(ref, ref, self.zsend.at[what, d, j], self.zrecv.at[what, d, j], to)

    def ycopy(self, hop, d, q, received):
        way = 1 if d == 0 else -1
        dy = -way * (hop + 1) if received else -way * hop
        ref = self.rows.at[self.at(self.zq(q), dy), 0]
        if hop == 1:
            ref = ref.at[pl.ds(0, 64)] if d == 0 else ref.at[pl.ds(64, ROWS - 64)]
        to = self.place.along_y(way)
        return remote(ref, ref, self.ysend.at[hop, d, q], self.yrecv.at[hop, d, q], to)

    def start(self, one):
        one.start()
        self.sent.append(one)

    def out_y(self, q):
        self.start(self.ycopy(0, 0, q, False))
        self.start(self.ycopy(0, 1, q, False))

    def on_y(self, q):
        self.ycopy(0, 0, q, True).wait_recv()
        self.start(self.ycopy(1, 0, q, False))
        self.ycopy(0, 1, q, True).wait_recv()
        self.start(self.ycopy(1, 1, q, False))

    def done(self, q):
        self.ycopy(1, 0, q, True).wait_recv()
        self.ycopy(1, 1, q, True).wait_recv()
        zz = self.zq(q)
        for dy in range(NY):
            self.give(self.at(zz, dy))

    def hops(self, j):
        return (0, 1) if j < HALF - 1 else (0,)

    def along_z(self, what, j):
        for d in self.hops(j):
            self.zcopy(what, d, j, True).wait_recv()
            if j + 2 < HALF - d:
                self.start(self.zcopy(what, d, j + 2, False))
        return [1 + 2 * j + d for d in self.hops(j)]

    def begin(self, what):
        for j in range(2):
            for d in range(2):
                self.start(self.zcopy(what, d, j, False))

    def run(self, collect):
        self.begin(0)
        self.begin(1)
        self.out_y(0)
        self.take(self.at(self.place.z, 0))
        groups = [[0]]
        for j in range(HALF + 4):
            if j < HALF:
                group = self.along_z(0, j)
                for q in group:
                    self.out_y(q)
                groups.append(group)
            if 0 < j <= HALF:
                for q in self.along_z(1, j - 1):
                    self.take(self.at(self.zq(q), 0))
            if j == HALF:
                collect.first()
            if j < len(groups):
                for q in groups[j]:
                    self.on_y(q)
            if j == HALF + 1:
                collect.second()
            if 0 <= j - 2 < len(groups):
                for q in groups[j - 2]:
                    self.done(q)
        for one in self.sent:
            one.wait_send()


class Collect:
    def __init__(self, place, tiles, summed, out, into, relay, last, send, recv):
        self.place, self.tiles, self.summed = place, tiles, summed
        self.out, self.into, self.relay, self.last = out, into, relay, last
        self.send, self.recv = send, recv
        self.sent = []

    def copy(self, hop, d):
        src, dst = (
            (self.out.at[d], self.into.at[d]),
            (self.out.at[2, d], self.relay.at[d]),
            (self.relay.at[d], self.last.at[d]),
        )[hop]
        to = self.place.along_y(1 if d == 0 else -1)
        return remote(src, dst, self.send.at[hop, d], self.recv.at[hop, d], to)

    def start(self, hop, d):
        one = self.copy(hop, d)
        one.start()
        self.sent.append(one)

    def first(self):
        for n in (2, 0, 1):
            for s in range(CAP):
                k = self.tiles[n * CAP + s]
                for b in range(8):
                    self.out[n, s, b * 16 : (b + 1) * 16, :] = self.summed[k * 8 + b]
            if n == 2:
                self.start(1, 0)
                self.start(1, 1)
            else:
                self.start(0, n)

    def second(self):
        for d in range(2):
            self.copy(1, d).wait_recv()
            self.start(2, d)

    def finish(self):
        for hop in (0, 2):
            for d in range(2):
                self.copy(hop, d).wait_recv()
        for one in self.sent:
            one.wait_send()

    def grad(self, s, b):
        block = slice(b * 16, (b + 1) * 16)
        value = self.summed[self.tiles[3 * CAP + s] * 8 + b].astype(F32)
        for other in (self.into[0, s, block, :], self.into[1, s, block, :], self.last[s, block, :]):
            value = value + other.astype(F32)
        return value


def dequantize(fscale, sscale, fcodes, scodes, smap, umap, exact, rounded):
    for a, (codes, table, scale) in enumerate(((fcodes, smap, fscale), (scodes, umap, sscale))):
        low_table = jnp.broadcast_to(table[0:1, :], (16, TB))
        high_table = jnp.broadcast_to(table[1:2, :], (16, TB))
        for s in range(CAP):
            for b in range(TB * TB // QB):
                block = slice(b * 16, (b + 1) * 16)
                code = codes[s, block, :]
                low = jnp.bitwise_and(code, TB - 1)
                value = jnp.where(
                    code < TB,
                    jnp.take_along_axis(low_table, low, axis=1, mode="promise_in_bounds"),
                    jnp.take_along_axis(high_table, low, axis=1, mode="promise_in_bounds"),
                )
                value = value * scale[s, b]
                exact[a, s, block, :] = value
                rounded[s, a, block, :] = value.astype(BF16)


def kernel(
    list_ref,
    slots_ref,
    exact_ref,
    rounded_ref,
    input_ref,
    grad_ref,
    gate_ref,
    up_ref,
    hgrad_ref,
    update_ref,
    first_ref,
    second_ref,
    left,
    right,
    parts,
    states,
    pool,
    rows,
    summed,
    old_kept,
    sum_kept,
    oz,
    iz,
    p1,
    q1,
    p2,
    q2,
    pz,
    qz,
    cout,
    cinto,
    crelay,
    clast,
    gsend,
    grecv,
    osend,
    orecv,
    esend,
    erecv,
    psend,
    precv,
    zsend,
    zrecv,
    ysend,
    yrecv,
    csend,
    crecv,
):
    place = Place()
    barrier = pltpu.get_barrier_semaphore()
    near = [place.partner()]
    for d in (1, -1):
        near += [place.along_x(d), place.along_y(d), place.along_z(d), place.along_z(2 * d)]
    for device in near:
        pl.semaphore_signal(barrier, inc=1, device_id=device, device_id_type=MESH)

    shared = Pool(place, pool, osend, orecv)
    pool[pl.ds(place.y * CAP, CAP)] = rounded_ref[...]
    pool[NY * CAP] = jnp.zeros((2, TB, TB), BF16)
    gather = Gather(place, left, right, gsend, grecv)
    for j in range(OWN):
        right[2 * HB + place.t * OWN + j] = grad_ref[:, j * TB : (j + 1) * TB]
    pl.semaphore_wait(barrier, len(near))
    shared.start(0)
    gather.begin(0)
    gather.begin(1)
    for j in range(OWN):
        left[place.t * OWN + j] = input_ref[:, j * TB : (j + 1) * TB].T
    gather.begin(2)
    gather.begin(3)

    def activations(i):
        for h in range(4 * i, 4 * i + 4):
            cols = slice(h * TB, (h + 1) * TB)
            gate = gate_ref[:, cols].astype(F32)
            up = up_ref[:, cols].astype(F32)
            grad = hgrad_ref[:, cols].astype(F32)
            sigmoid = 1.0 / (1.0 + jnp.exp(-gate))
            silu = gate * sigmoid
            left[WB + h] = (silu * up).astype(BF16).T
            right[h] = (grad * up * sigmoid * (1.0 + gate * (1.0 - sigmoid))).astype(BF16)
            right[HB + h] = (grad * silu).astype(BF16)

    def fill(k, carry):
        slot = slots_ref[k]
        near = lax.shift_right_logical(slot, 3) == place.z
        mine = jnp.where(near, jnp.bitwise_and(slot, NY * CAP - 1), NY * CAP)
        for a in range(2):
            states[a, pl.ds(pl.multiple_of(k * TB, TB), TB), :] = pool[mine, a]
        return carry

    olds = Olds(place, states, oz, iz, esend, erecv, old_kept)
    activations(0)
    shared.start(1)
    activations(1)
    gather.step(0)
    shared.finish()
    lax.fori_loop(0, TILES, fill, 0)
    for i in range(HALF):
        olds.slot(i)
        gather.step(i + 1)
        if i + 2 < HB // 4:
            activations(i + 2)

    def find(k, found):
        slot = slots_ref[k]
        return tuple(jnp.where(slot == one, k, old) for one, old in zip(wanted, found))

    wanted = [
        (place.z * NY + up_to(place.y + NY + dy, NY)) * CAP + s for dy in (1, -1, 2, 0) for s in range(CAP)
    ]
    tiles = lax.fori_loop(0, TILES, find, (jnp.int32(TILES),) * len(wanted))
    summed[...] = jnp.zeros(summed.shape, BF16)
    olds.finish()
    gather.finish()

    def multiply(k, carry):
        width, hidden, matrix = list_ref[0, k], list_ref[1, k], list_ref[2, k]
        li = jnp.where(matrix == 2, WB + hidden, width)
        ri = jnp.where(matrix == 2, 2 * HB + width, jnp.where(matrix == 1, HB + hidden, hidden))
        tile = jnp.dot(left[li], right[ri], preferred_element_type=F32)
        parts[0, pl.ds(pl.multiple_of(k * TB, TB), TB), :] = tile.astype(BF16)
        return carry

    lax.fori_loop(0, TILES, multiply, 0, unroll=4)

    sums = Scatter(place, parts, (p1, q1, p2, q2, pz, qz), psend, precv, sum_kept)
    for i in range(HALF + 2 * LAG):
        sums.slot(i)
    sums.finish()

    def moments(first_old, second_old, grad):
        first = BETA_FIRST * first_old + (1.0 - BETA_FIRST) * grad
        second = BETA_SECOND * second_old + (1.0 - BETA_SECOND) * grad * grad
        return first, second

    grad = sum_kept[0]
    first, second = moments(old_kept[0], old_kept[1], grad)
    first_hat = first / (1.0 - BETA_FIRST**STEP)
    second_hat = second / (1.0 - BETA_SECOND**STEP)
    rows[place.dp, 0] = (first_hat / (jnp.sqrt(second_hat) + EPSILON)).astype(BF16)
    rows[place.dp, 1] = grad.astype(BF16)

    def give(dp):
        update_ref[pl.ds(pl.multiple_of(dp * ROWS, 16), ROWS), :] = rows[dp, 0]

    def take(dp):
        summed[pl.ds(dp * (ROWS // 16), ROWS // 16)] = rows[dp, 1].reshape(ROWS // 16, 16, TB)

    collect = Collect(place, tiles, summed, cout, cinto, crelay, clast, csend, crecv)
    Spread(place, rows, zsend, zrecv, ysend, yrecv, give, take).run(collect)
    collect.finish()
    for s in range(CAP):
        for b in range(8):
            block = slice(b * 16, (b + 1) * 16)
            grad = collect.grad(s, b)
            first, second = moments(exact_ref[0, s, block, :], exact_ref[1, s, block, :], grad)
            for r in range(16):
                lanes = slice((b * 16 + r) * TB, (b * 16 + r + 1) * TB)
                first_ref[s : s + 1, lanes] = first[r : r + 1, :]
                second_ref[s : s + 1, lanes] = second[r : r + 1, :]


def body(
    layer_input,
    output_grad,
    gate_pre,
    up_pre,
    hidden_grad,
    tile_list,
    tile_slots,
    first_codes,
    second_codes,
    first_absmax,
    second_absmax,
    signed_map,
    unsigned_map,
):
    vmem = pl.BlockSpec(memory_space=pltpu.VMEM)
    smem = pl.BlockSpec(memory_space=pltpu.SMEM)

    def scatter_shapes(n):
        one = [pltpu.VMEM((2, HALF, n, ROWS, TB), BF16)] * 2
        two = [pltpu.VMEM((2, HALF, 2, n, ROWS, TB), BF16)] * 2
        return one + two + one

    exact, rounded = pl.pallas_call(
        dequantize,
        out_shape=(
            jax.ShapeDtypeStruct((2, CAP, TB, TB), F32),
            jax.ShapeDtypeStruct((CAP, 2, TB, TB), BF16),
        ),
        in_specs=[smem] * 2 + [vmem] * 4,
        out_specs=[vmem] * 2,
    )(
        first_absmax[0],
        second_absmax[0],
        first_codes.reshape(CAP, TB, TB),
        second_codes.reshape(CAP, TB, TB),
        signed_map.reshape(2, TB),
        unsigned_map.reshape(2, TB),
    )
    dma = pltpu.SemaphoreType.DMA
    update, first, second = pl.pallas_call(
        kernel,
        out_shape=(
            jax.ShapeDtypeStruct((TILES * TB, TB), BF16),
            jax.ShapeDtypeStruct((CAP, TB * TB), F32),
            jax.ShapeDtypeStruct((CAP, TB * TB), F32),
        ),
        in_specs=[smem] * 2 + [vmem] * 7,
        out_specs=[vmem] * 3,
        scratch_shapes=[
            pltpu.VMEM((WB + HB, TB, TB), BF16),
            pltpu.VMEM((WB + 2 * HB, TB, TB), BF16),
            pltpu.VMEM((1, TILES * TB, TB), BF16),
            pltpu.VMEM((2, TILES * TB, TB), BF16),
            pltpu.VMEM((NY * CAP + 1, 2, TB, TB), BF16),
            pltpu.VMEM((NY * NZ, 2, ROWS, TB), BF16),
            pltpu.VMEM(((TILES + 1) * 8, 16, TB), BF16),
            pltpu.VMEM((2, ROWS, TB), F32),
            pltpu.VMEM((1, ROWS, TB), F32),
        ]
        + [pltpu.VMEM((2, HALF, 2, ROWS, TB), BF16)] * 2
        + scatter_shapes(1)
        + [
            pltpu.VMEM((3, CAP, TB, TB), BF16),
            pltpu.VMEM((2, CAP, TB, TB), BF16),
            pltpu.VMEM((2, TB, TB), BF16),
            pltpu.VMEM((2, TB, TB), BF16),
        ]
        + [dma((7, 4))] * 2
        + [dma((2, 2))] * 2
        + [dma((2, HALF))] * 2
        + [dma((3, 2, HALF))] * 2
        + [dma((2, 2, HALF))] * 2
        + [dma((2, 2, NZ))] * 2
        + [dma((3, 2))] * 2,
        compiler_params=pltpu.CompilerParams(
            collective_id=0, has_side_effects=True, vmem_limit_bytes=60 * 1024 * 1024
        ),
    )(
        tile_list.T,
        tile_slots,
        exact,
        rounded,
        layer_input,
        output_grad,
        gate_pre,
        up_pre,
        hidden_grad,
    )
    return (
        update.reshape(TILES, TB, TB),
        first.reshape(1, CAP, TB * TB),
        second.reshape(1, CAP, TB * TB),
    )


def solution(mesh):
    in_specs = (
        P("dp", "tensor"),
        P("dp", "tensor"),
        P("dp", "tensor"),
        P("dp", "tensor"),
        P("dp", "tensor"),
        P("tensor", None),
        P("tensor"),
        P("tensor", "dp", None),
        P("tensor", "dp", None),
        P("tensor", "dp", None),
        P("tensor", "dp", None),
        P(),
        P(),
    )
    out_specs = (P("tensor", None, None), P("tensor", "dp", None), P("tensor", "dp", None))
    return jax.shard_map(body, mesh=mesh, in_specs=in_specs, out_specs=out_specs, check_vma=False)
```

```python
import functools

import jax
import jax.numpy as jnp
from jax import lax
from jax.experimental import pallas as pl
from jax.experimental.pallas import tpu as pltpu
from jax.sharding import PartitionSpec as P

CAP = 2
TB = 128
QB = 2048
STEP = 10
BETA_FIRST = 0.9
BETA_SECOND = 0.99
EPSILON = 1e-08

NX, NY, NZ = 4, 4, 16
TILES = 56
WB = 64
HB = 28
OWN = WB // 8
ROWS = TILES * TB // (NY * NZ)
HALF = NZ // 2
LAG = 2
EARLY = 4
MESH = pl.DeviceIdType.MESH
F32, BF16 = jnp.float32, jnp.bfloat16


def up_to(value, size):
    return lax.rem(value, size)


class Place:
    def __init__(self):
        dp, t = lax.axis_index("dp"), lax.axis_index("tensor")
        self.dp, self.t = dp, t
        self.z, self.y = dp // NY, lax.rem(dp, NY)
        self.x, self.c = t // 2, lax.rem(t, 2)

    def along_x(self, d):
        return (self.dp, up_to(self.x + NX + d, NX) * 2 + self.c)

    def partner(self):
        return (self.dp, self.x * 2 + 1 - self.c)

    def along_y(self, d):
        return (self.z * NY + up_to(self.y + NY + d, NY), self.t)

    def along_z(self, d):
        return (up_to(self.z + NZ + d, NZ) * NY + self.y, self.t)


def remote(src, dst, send, recv, device):
    return pltpu.make_async_remote_copy(
        src_ref=src, dst_ref=dst, send_sem=send, recv_sem=recv, device_id=device, device_id_type=MESH
    )


def moments(first_old, second_old, grad):
    first = BETA_FIRST * first_old + (1.0 - BETA_FIRST) * grad
    second = BETA_SECOND * second_old + (1.0 - BETA_SECOND) * grad * grad
    return first, second


def leap(d, j):
    return min(2, HALF - d - j)


class Gather:
    def __init__(self, place, left, right, send, recv):
        self.place, self.left, self.right, self.send, self.recv = place, left, right, send, recv
        self.sent = []

    def piece(self, d, other, p):
        pc = self.place
        core = 1 - pc.c if other else pc.c
        owner = up_to(pc.x + NX + d, NX) * 2 + core
        if p < 2:
            return self.right.at[pl.ds(2 * HB + owner * OWN + p * 4, 4)]
        return self.left.at[pl.ds(owner * OWN + (p - 2) * 4, 4)]

    def copy(self, route, p):
        pc = self.place
        shift = {0: 0, 1: 0, 2: 0, 3: -1, 4: 1, 5: -1 if p % 2 == 0 else 1, 6: 2}[route]
        to = {0: pc.along_x(1), 1: pc.along_x(-1), 5: pc.along_x(1 if p % 2 == 0 else -1)}.get(route)
        to = pc.partner() if to is None else to
        block = self.piece(shift, False, p)
        return remote(block, block, self.send.at[route, p], self.recv.at[route, p], to)

    def start(self, route, p):
        one = self.copy(route, p)
        one.start()
        self.sent.append(one)

    def arrived(self, route, p):
        shift, other = {
            0: (-1, False),
            1: (1, False),
            2: (0, True),
            3: (-1, True),
            4: (1, True),
            5: (2, False),
            6: (2, True),
        }[route]
        block = self.piece(shift, other, p)
        remote(
            block, block, self.send.at[route, p], self.recv.at[route, p], self.place.partner()
        ).wait_recv()

    def begin(self, p):
        for route in (0, 1, 2):
            self.start(route, p)

    def step(self, i):
        if i < 4:
            self.arrived(0, i)
            if i % 2 == 0:
                self.start(5, i)
            self.start(3, i)
            self.arrived(1, i)
            if i % 2 == 1:
                self.start(5, i)
            self.start(4, i)
        elif i < 8:
            self.arrived(5, i - 4)
            self.start(6, i - 4)

    def finish(self):
        for p in range(4):
            for route in (2, 3, 4, 6):
                self.arrived(route, p)
        for one in self.sent:
            one.wait_send()


class Scatter:
    def __init__(self, place, source, bufs, send, recv, kept, make):
        self.make = make
        self.place, self.source, self.send, self.recv, self.kept = place, source, send, recv, kept
        self.s1, self.r1, self.s2, self.r2, self.sz, self.rz = bufs
        self.sent = []

    def own(self, zz, dy):
        yy = up_to(self.place.y + NY + dy, NY)
        start = pl.multiple_of((zz * NY + yy) * ROWS, 16)
        return self.source[:, pl.ds(start, ROWS), :]

    def zs(self, j):
        z = self.place.z
        return up_to(z + HALF - j, NZ), up_to(z + NZ - (HALF - 1 - j), NZ)

    def copy(self, kind, d, j):
        src, dst = ((self.s1, self.r1), (self.s2, self.r2), (self.sz, self.rz))[kind]
        way = 1 if d == 0 else -1
        to = self.place.along_z(way * leap(d, j)) if kind == 2 else self.place.along_y(way)
        return remote(src.at[d, j], dst.at[d, j], self.send.at[kind, d, j], self.recv.at[kind, d, j], to)

    def start(self, kind, d, j):
        one = self.copy(kind, d, j)
        one.start()
        self.sent.append(one)

    def first(self, j):
        za, zb = self.zs(j)
        self.make(za)
        self.make(zb)
        self.s1[0, j] = self.own(za, 2)
        self.start(0, 0, j)
        self.s1[1, j] = self.own(zb, 2)
        self.start(0, 1, j)

    def second(self, j):
        za, zb = self.zs(j)
        self.s2[0, j, 1] = self.own(zb, 1)
        self.s2[1, j, 0] = self.own(za, -1)
        self.copy(0, 0, j).wait_recv()
        self.s2[0, j, 0] = (self.r1[0, j].astype(F32) + self.own(za, 1).astype(F32)).astype(BF16)
        self.start(1, 0, j)
        self.copy(0, 1, j).wait_recv()
        self.s2[1, j, 1] = (self.r1[1, j].astype(F32) + self.own(zb, -1).astype(F32)).astype(BF16)
        self.start(1, 1, j)

    def third(self, j):
        za, zb = self.zs(j)
        self.copy(1, 0, j).wait_recv()
        self.copy(1, 1, j).wait_recv()
        sum_a = self.own(za, 0).astype(F32) + self.r2[0, j, 0].astype(F32) + self.r2[1, j, 0].astype(F32)
        sum_b = self.own(zb, 0).astype(F32) + self.r2[0, j, 1].astype(F32) + self.r2[1, j, 1].astype(F32)
        if j > 1:
            self.copy(2, 0, j - 2).wait_recv()
            sum_a = sum_a + self.rz[0, j - 2].astype(F32)
        self.sz[0, j] = sum_a.astype(BF16)
        self.start(2, 0, j)
        if j > 1:
            self.copy(2, 1, j - 2).wait_recv()
            sum_b = sum_b + self.rz[1, j - 2].astype(F32)
        if j < HALF - 1:
            self.sz[1, j] = sum_b.astype(BF16)
            self.start(2, 1, j)
        else:
            self.kept[...] = sum_b

    def slot(self, i):
        if i < HALF:
            self.first(i)
        if 0 <= i - LAG < HALF:
            self.second(i - LAG)
        if 0 <= i - 2 * LAG < HALF:
            self.third(i - 2 * LAG)

    def finish(self):
        for d, j in ((0, HALF - 2), (1, HALF - 2), (0, HALF - 1)):
            self.copy(2, d, j).wait_recv()
            self.kept[...] = self.kept[...] + self.rz[d, j].astype(F32)
        for one in self.sent:
            one.wait_send()


class Pool:
    def __init__(self, place, pool, send, recv):
        self.place, self.pool, self.send, self.recv = place, pool, send, recv
        self.sent = []

    def copy(self, hop, d, received):
        way = 1 if d == 0 else -1
        back = -way * (hop + 1) if received else -way * hop
        yy = up_to(self.place.y + NY + back, NY)
        ref = self.pool.at[pl.ds(yy * CAP, CAP)] if hop == 0 else self.pool.at[yy * CAP + d]
        return remote(ref, ref, self.send.at[hop, d], self.recv.at[hop, d], self.place.along_y(way))

    def start(self, hop):
        for d in range(2):
            if hop == 1:
                self.copy(0, d, True).wait_recv()
            one = self.copy(hop, d, False)
            one.start()
            self.sent.append(one)

    def finish(self):
        for d in range(2):
            self.copy(1, d, True).wait_recv()
        for one in self.sent:
            one.wait_send()


class Olds:
    def __init__(self, place, states, out, into, send, recv, kept):
        self.place, self.states, self.out, self.into = place, states, out, into
        self.send, self.recv, self.kept = send, recv, kept
        self.sent = []

    def copy(self, d, j):
        to = self.place.along_z(leap(d, j) if d == 0 else -leap(d, j))
        return remote(self.out.at[d, j], self.into.at[d, j], self.send.at[d, j], self.recv.at[d, j], to)

    def own(self, zz):
        start = pl.multiple_of((zz * NY + self.place.y) * ROWS, 16)
        return self.states[:, pl.ds(start, ROWS), :].astype(F32)

    def slot(self, j):
        z = self.place.z
        far = (up_to(z + HALF - j, NZ), up_to(z + NZ - (HALF - 1 - j), NZ))
        for d in range(2):
            value = self.own(far[d])
            if j > 1:
                self.copy(d, j - 2).wait_recv()
                value = value + self.into[d, j - 2].astype(F32)
            if d == 1 and j == HALF - 1:
                self.kept[...] = value
            else:
                self.out[d, j] = value.astype(BF16)
                one = self.copy(d, j)
                one.start()
                self.sent.append(one)

    def finish(self):
        for d, j in ((0, HALF - 2), (1, HALF - 2), (0, HALF - 1)):
            self.copy(d, j).wait_recv()
            self.kept[...] = self.kept[...] + self.into[d, j].astype(F32)
        for one in self.sent:
            one.wait_send()


class Spread:
    def __init__(self, place, rows, zsend, zrecv, ysend, yrecv, give, take):
        self.place, self.rows, self.give, self.take = place, rows, give, take
        self.zsend, self.zrecv, self.ysend, self.yrecv = zsend, zrecv, ysend, yrecv
        self.sent = []

    def zq(self, q):
        z = self.place.z
        if q == 0:
            return z
        if q % 2 == 1:
            return up_to(z + NZ - 1 - (q - 1) // 2, NZ)
        return up_to(z + 1 + (q - 2) // 2, NZ)

    def at(self, zz, dy):
        return zz * NY + up_to(self.place.y + NY + dy, NY)

    def zcopy(self, what, d, j, received):
        z = self.place.z
        step = min(2, j + 1)
        back = j + 1 if received else j + 1 - step
        zz = up_to(z + NZ - back, NZ) if d == 0 else up_to(z + back, NZ)
        ref = self.rows.at[self.at(zz, 0), what]
        to = self.place.along_z(step if d == 0 else -step)
        return remote(ref, ref, self.zsend.at[what, d, j], self.zrecv.at[what, d, j], to)

    def ycopy(self, hop, d, q, received):
        way = 1 if d == 0 else -1
        dy = -way * (hop + 1) if received else -way * hop
        ref = self.rows.at[self.at(self.zq(q), dy), 0]
        if hop == 1:
            ref = ref.at[pl.ds(0, 64)] if d == 0 else ref.at[pl.ds(64, ROWS - 64)]
        to = self.place.along_y(way)
        return remote(ref, ref, self.ysend.at[hop, d, q], self.yrecv.at[hop, d, q], to)

    def start(self, one):
        one.start()
        self.sent.append(one)

    def out_y(self, q):
        self.start(self.ycopy(0, 0, q, False))
        self.start(self.ycopy(0, 1, q, False))

    def on_y(self, q):
        self.ycopy(0, 0, q, True).wait_recv()
        self.start(self.ycopy(1, 0, q, False))
        self.ycopy(0, 1, q, True).wait_recv()
        self.start(self.ycopy(1, 1, q, False))

    def done(self, q):
        self.ycopy(1, 0, q, True).wait_recv()
        self.ycopy(1, 1, q, True).wait_recv()
        zz = self.zq(q)
        for dy in range(NY):
            self.give(self.at(zz, dy))

    def hops(self, j):
        return (0, 1) if j < HALF - 1 else (0,)

    def along_z(self, what, j):
        for d in self.hops(j):
            self.zcopy(what, d, j, True).wait_recv()
            if j + 2 < HALF - d:
                self.start(self.zcopy(what, d, j + 2, False))
        return [1 + 2 * j + d for d in self.hops(j)]

    def begin(self, what):
        for j in range(2):
            for d in range(2):
                self.start(self.zcopy(what, d, j, False))

    def run(self, collect):
        self.begin(0)
        self.begin(1)
        self.out_y(0)
        self.take(self.at(self.place.z, 0))
        groups = [[0]]
        for j in range(HALF + 4):
            if j < HALF:
                group = self.along_z(0, j)
                for q in group:
                    self.out_y(q)
                groups.append(group)
            if 0 < j <= HALF:
                for q in self.along_z(1, j - 1):
                    self.take(self.at(self.zq(q), 0))
            if j == HALF:
                collect.first()
            if j < len(groups):
                for q in groups[j]:
                    self.on_y(q)
            if j == HALF + 1:
                collect.second()
            if 0 <= j - 2 < len(groups):
                for q in groups[j - 2]:
                    self.done(q)
        for one in self.sent:
            one.wait_send()


class Collect:
    def __init__(self, place, tiles, summed, out, into, relay, last, send, recv):
        self.place, self.tiles, self.summed = place, tiles, summed
        self.out, self.into, self.relay, self.last = out, into, relay, last
        self.send, self.recv = send, recv
        self.sent = []

    def copy(self, hop, d):
        src, dst = (
            (self.out.at[d], self.into.at[d]),
            (self.out.at[2, d], self.relay.at[d]),
            (self.relay.at[d], self.last.at[d]),
        )[hop]
        to = self.place.along_y(1 if d == 0 else -1)
        return remote(src, dst, self.send.at[hop, d], self.recv.at[hop, d], to)

    def start(self, hop, d):
        one = self.copy(hop, d)
        one.start()
        self.sent.append(one)

    def first(self):
        for n in (2, 0, 1):
            for s in range(CAP):
                k = self.tiles[n * CAP + s]
                for b in range(8):
                    self.out[n, s, b * 16 : (b + 1) * 16, :] = self.summed[k * 8 + b]
            if n == 2:
                self.start(1, 0)
                self.start(1, 1)
            else:
                self.start(0, n)

    def second(self):
        for d in range(2):
            self.copy(1, d).wait_recv()
            self.start(2, d)

    def finish(self):
        for hop in (0, 2):
            for d in range(2):
                self.copy(hop, d).wait_recv()
        for one in self.sent:
            one.wait_send()

    def grad(self, s, b):
        block = slice(b * 16, (b + 1) * 16)
        value = self.summed[self.tiles[3 * CAP + s] * 8 + b].astype(F32)
        for other in (self.into[0, s, block, :], self.into[1, s, block, :], self.last[s, block, :]):
            value = value + other.astype(F32)
        return value


def dequantize(fscale, sscale, fcodes, scodes, smap, umap, exact, rounded):
    for a, (codes, table, scale) in enumerate(((fcodes, smap, fscale), (scodes, umap, sscale))):
        low_table = jnp.broadcast_to(table[0:1, :], (16, TB))
        high_table = jnp.broadcast_to(table[1:2, :], (16, TB))
        for s in range(CAP):
            for b in range(TB * TB // QB):
                block = slice(b * 16, (b + 1) * 16)
                code = codes[block, s, :]
                low = jnp.bitwise_and(code, TB - 1)
                value = jnp.where(
                    code < TB,
                    jnp.take_along_axis(low_table, low, axis=1, mode="promise_in_bounds"),
                    jnp.take_along_axis(high_table, low, axis=1, mode="promise_in_bounds"),
                )
                value = value * scale[s, b]
                exact[a, s, block, :] = value
                rounded[s, a, block, :] = value.astype(BF16)


def kernel(
    list_ref,
    slots_ref,
    rounded_ref,
    input_ref,
    grad_ref,
    gate_ref,
    up_ref,
    hgrad_ref,
    update_ref,
    grad_out_ref,
    left,
    right,
    parts,
    states,
    pool,
    rows,
    summed,
    old_kept,
    sum_kept,
    oz,
    iz,
    p1,
    q1,
    p2,
    q2,
    pz,
    qz,
    cout,
    cinto,
    crelay,
    clast,
    gsend,
    grecv,
    osend,
    orecv,
    esend,
    erecv,
    psend,
    precv,
    zsend,
    zrecv,
    ysend,
    yrecv,
    csend,
    crecv,
    out_sem,
):
    place = Place()
    barrier = pltpu.get_barrier_semaphore()
    near = [place.partner()]
    for d in (1, -1):
        near += [place.along_x(d), place.along_y(d), place.along_z(d), place.along_z(2 * d)]
    for device in near:
        pl.semaphore_signal(barrier, inc=1, device_id=device, device_id_type=MESH)

    shared = Pool(place, pool, osend, orecv)
    pool[pl.ds(place.y * CAP, CAP)] = rounded_ref[...]
    pool[NY * CAP] = jnp.zeros((2, TB, TB), BF16)
    gather = Gather(place, left, right, gsend, grecv)
    for j in range(OWN):
        right[2 * HB + place.t * OWN + j] = grad_ref[:, j * TB : (j + 1) * TB]
    pl.semaphore_wait(barrier, len(near))
    shared.start(0)
    gather.begin(0)
    gather.begin(1)
    for j in range(OWN):
        left[place.t * OWN + j] = input_ref[:, j * TB : (j + 1) * TB].T
    gather.begin(2)
    gather.begin(3)

    def activations(i):
        for h in range(4 * i, 4 * i + 4):
            cols = slice(h * TB, (h + 1) * TB)
            gate = gate_ref[:, cols].astype(F32)
            up = up_ref[:, cols].astype(F32)
            grad = hgrad_ref[:, cols].astype(F32)
            sigmoid = 1.0 / (1.0 + jnp.exp(-gate))
            silu = gate * sigmoid
            left[WB + h] = (silu * up).astype(BF16).T
            right[h] = (grad * up * sigmoid * (1.0 + gate * (1.0 - sigmoid))).astype(BF16)
            right[HB + h] = (grad * silu).astype(BF16)

    def fill(k, carry):
        slot = slots_ref[k]
        near = lax.shift_right_logical(slot, 3) == place.z
        mine = jnp.where(near, jnp.bitwise_and(slot, NY * CAP - 1), NY * CAP)
        for a in range(2):
            states[a, pl.ds(pl.multiple_of(k * TB, TB), TB), :] = pool[mine, a]
        return carry

    olds = Olds(place, states, oz, iz, esend, erecv, old_kept)
    activations(0)
    shared.start(1)
    activations(1)
    gather.step(0)
    shared.finish()
    lax.fori_loop(0, TILES, fill, 0)
    for i in range(HALF):
        if i < EARLY:
            olds.slot(i)
        gather.step(i + 1)
        if i + 2 < HB // 4:
            activations(i + 2)

    def find(k, found):
        slot = slots_ref[k]
        return tuple(jnp.where(slot == one, k, old) for one, old in zip(wanted, found))

    wanted = [
        (place.z * NY + up_to(place.y + NY + dy, NY)) * CAP + s for dy in (1, -1, 2, 0) for s in range(CAP)
    ]
    tiles = lax.fori_loop(0, TILES, find, (jnp.int32(TILES),) * len(wanted))
    summed[...] = jnp.zeros(summed.shape, BF16)
    gather.finish()

    def multiply(k, carry):
        width, hidden, matrix = list_ref[0, k], list_ref[1, k], list_ref[2, k]
        li = jnp.where(matrix == 2, WB + hidden, width)
        ri = jnp.where(matrix == 2, 2 * HB + width, jnp.where(matrix == 1, HB + hidden, hidden))
        tile = jnp.dot(left[li], right[ri], preferred_element_type=F32)
        parts[0, pl.ds(pl.multiple_of(k * TB, TB), TB), :] = tile.astype(BF16)
        return carry

    def products(zz):
        start = NY * ROWS * zz // TB
        lax.fori_loop(0, NY * ROWS // TB + 1, lambda i, carry: multiply(start + i, carry), 0, unroll=True)

    sums = Scatter(place, parts, (p1, q1, p2, q2, pz, qz), psend, precv, sum_kept, products)
    for i in range(HALF + 2 * LAG):
        sums.slot(i)
        if i + EARLY < HALF:
            olds.slot(i + EARLY)
    olds.finish()
    sums.finish()

    grad = sum_kept[0]
    first, second = moments(old_kept[0], old_kept[1], grad)
    first_hat = first / (1.0 - BETA_FIRST**STEP)
    second_hat = second / (1.0 - BETA_SECOND**STEP)
    rows[place.dp, 0] = (first_hat / (jnp.sqrt(second_hat) + EPSILON)).astype(BF16)
    rows[place.dp, 1] = grad.astype(BF16)

    gives = []

    def give(dp):
        where = pl.ds(pl.multiple_of(dp * ROWS, 16), ROWS)
        one = pltpu.make_async_copy(rows.at[dp, 0], update_ref.at[where], out_sem.at[len(gives)])
        one.start()
        gives.append(one)

    def take(dp):
        summed[pl.ds(dp * (ROWS // 16), ROWS // 16)] = rows[dp, 1].reshape(ROWS // 16, 16, TB)

    collect = Collect(place, tiles, summed, cout, cinto, crelay, clast, csend, crecv)
    Spread(place, rows, zsend, zrecv, ysend, yrecv, give, take).run(collect)
    collect.finish()
    for s in range(CAP):
        for b in range(8):
            grad_out_ref[s, b * 16 : (b + 1) * 16, :] = collect.grad(s, b)
    for one in gives:
        one.wait()


def finish(update_ref, grad_ref, exact_ref, out_ref, first_ref, second_ref, buffer, into, out):
    count = into.shape[0]
    size = TILES * TB // count
    copies = []
    for i in range(count):
        where = pl.ds(i * size, size)
        one = pltpu.make_async_copy(update_ref.at[where], buffer.at[where], into.at[i])
        one.start()
        copies.append((one, pltpu.make_async_copy(buffer.at[where], out_ref.at[where], out.at[i])))
    for one, two in copies:
        one.wait()
        two.start()
    for s in range(CAP):
        for b in range(16):
            block = slice(b * 8, (b + 1) * 8)
            first, second = moments(exact_ref[0, s, block, :], exact_ref[1, s, block, :], grad_ref[s, block, :])
            first_ref[block, s, :] = first
            second_ref[block, s, :] = second
    for one, two in copies:
        two.wait()


def body(
    layer_input,
    output_grad,
    gate_pre,
    up_pre,
    hidden_grad,
    tile_list,
    tile_slots,
    first_codes,
    second_codes,
    first_absmax,
    second_absmax,
    signed_map,
    unsigned_map,
):
    vmem = pl.BlockSpec(memory_space=pltpu.VMEM)
    smem = pl.BlockSpec(memory_space=pltpu.SMEM)

    def scatter_shapes(n):
        one = [pltpu.VMEM((2, HALF, n, ROWS, TB), BF16)] * 2
        two = [pltpu.VMEM((2, HALF, 2, n, ROWS, TB), BF16)] * 2
        return one + two + one

    exact, rounded = pl.pallas_call(
        dequantize,
        out_shape=(
            jax.ShapeDtypeStruct((2, CAP, TB, TB), F32),
            jax.ShapeDtypeStruct((CAP, 2, TB, TB), BF16),
        ),
        in_specs=[smem] * 2 + [vmem] * 4,
        out_specs=[vmem] * 2,
    )(
        first_absmax[0],
        second_absmax[0],
        first_codes.reshape(CAP, TB, TB).transpose(1, 0, 2),
        second_codes.reshape(CAP, TB, TB).transpose(1, 0, 2),
        signed_map.reshape(2, TB),
        unsigned_map.reshape(2, TB),
    )
    dma = pltpu.SemaphoreType.DMA
    update, grad = pl.pallas_call(
        kernel,
        out_shape=(
            jax.ShapeDtypeStruct((TILES * TB, TB), BF16),
            jax.ShapeDtypeStruct((CAP, TB, TB), F32),
        ),
        in_specs=[smem] * 2 + [vmem] * 6,
        out_specs=[pl.BlockSpec(memory_space=pl.ANY), vmem],
        scratch_shapes=[
            pltpu.VMEM((WB + HB, TB, TB), BF16),
            pltpu.VMEM((WB + 2 * HB, TB, TB), BF16),
            pltpu.VMEM((1, TILES * TB, TB), BF16),
            pltpu.VMEM((2, TILES * TB, TB), BF16),
            pltpu.VMEM((NY * CAP + 1, 2, TB, TB), BF16),
            pltpu.VMEM((NY * NZ, 2, ROWS, TB), BF16),
            pltpu.VMEM(((TILES + 1) * 8, 16, TB), BF16),
            pltpu.VMEM((2, ROWS, TB), F32),
            pltpu.VMEM((1, ROWS, TB), F32),
        ]
        + [pltpu.VMEM((2, HALF, 2, ROWS, TB), BF16)] * 2
        + scatter_shapes(1)
        + [
            pltpu.VMEM((3, CAP, TB, TB), BF16),
            pltpu.VMEM((2, CAP, TB, TB), BF16),
            pltpu.VMEM((2, TB, TB), BF16),
            pltpu.VMEM((2, TB, TB), BF16),
        ]
        + [dma((7, 4))] * 2
        + [dma((2, 2))] * 2
        + [dma((2, HALF))] * 2
        + [dma((3, 2, HALF))] * 2
        + [dma((2, 2, HALF))] * 2
        + [dma((2, 2, NZ))] * 2
        + [dma((3, 2))] * 2
        + [dma((NY * NZ,))],
        compiler_params=pltpu.CompilerParams(
            collective_id=0, has_side_effects=True, vmem_limit_bytes=60 * 1024 * 1024
        ),
    )(
        tile_list.T,
        tile_slots,
        rounded,
        layer_input,
        output_grad,
        gate_pre,
        up_pre,
        hidden_grad,
    )
    anywhere = pl.BlockSpec(memory_space=pl.ANY)
    update, first, second = pl.pallas_call(
        finish,
        out_shape=(
            jax.ShapeDtypeStruct((TILES * TB, TB), BF16),
            jax.ShapeDtypeStruct((TB, CAP, TB), F32),
            jax.ShapeDtypeStruct((TB, CAP, TB), F32),
        ),
        in_specs=[anywhere, vmem, vmem],
        out_specs=[anywhere, vmem, vmem],
        scratch_shapes=[pltpu.VMEM((TILES * TB, TB), BF16), dma((8,)), dma((8,))],
    )(update, grad, exact)
    return (
        update.reshape(TILES, TB, TB),
        first.transpose(1, 0, 2).reshape(1, CAP, TB * TB),
        second.transpose(1, 0, 2).reshape(1, CAP, TB * TB),
    )


def solution(mesh):
    in_specs = (
        P("dp", "tensor"),
        P("dp", "tensor"),
        P("dp", "tensor"),
        P("dp", "tensor"),
        P("dp", "tensor"),
        P("tensor", None),
        P("tensor"),
        P("tensor", "dp", None),
        P("tensor", "dp", None),
        P("tensor", "dp", None),
        P("tensor", "dp", None),
        P(),
        P(),
    )
    out_specs = (P("tensor", None, None), P("tensor", "dp", None), P("tensor", "dp", None))
    return jax.shard_map(body, mesh=mesh, in_specs=in_specs, out_specs=out_specs, check_vma=False)
```

```python
import functools

import jax
import jax.numpy as jnp
from jax import lax
from jax.experimental import pallas as pl
from jax.experimental.pallas import tpu as pltpu
from jax.sharding import PartitionSpec as P

CAP = 2
TB = 128
QB = 2048
STEP = 10
BETA_FIRST = 0.9
BETA_SECOND = 0.99
EPSILON = 1e-08

NX, NY, NZ = 4, 4, 16
TILES = 56
WB = 64
HB = 28
OWN = WB // 8
ROWS = TILES * TB // (NY * NZ)
HALF = NZ // 2
LAG = 2
EARLY = 4
MESH = pl.DeviceIdType.MESH
F32, BF16 = jnp.float32, jnp.bfloat16


def up_to(value, size):
    return lax.rem(value, size)


class Place:
    def __init__(self):
        dp, t = lax.axis_index("dp"), lax.axis_index("tensor")
        self.dp, self.t = dp, t
        self.z, self.y = dp // NY, lax.rem(dp, NY)
        self.x, self.c = t // 2, lax.rem(t, 2)

    def along_x(self, d):
        return (self.dp, up_to(self.x + NX + d, NX) * 2 + self.c)

    def partner(self):
        return (self.dp, self.x * 2 + 1 - self.c)

    def along_y(self, d):
        return (self.z * NY + up_to(self.y + NY + d, NY), self.t)

    def along_z(self, d):
        return (up_to(self.z + NZ + d, NZ) * NY + self.y, self.t)


def remote(src, dst, send, recv, device):
    return pltpu.make_async_remote_copy(
        src_ref=src, dst_ref=dst, send_sem=send, recv_sem=recv, device_id=device, device_id_type=MESH
    )


def moments(first_old, second_old, grad):
    first = BETA_FIRST * first_old + (1.0 - BETA_FIRST) * grad
    second = BETA_SECOND * second_old + (1.0 - BETA_SECOND) * grad * grad
    return first, second


def leap(d, j):
    return min(2, HALF - d - j)


class Gather:
    def __init__(self, place, left, right, send, recv):
        self.place, self.left, self.right, self.send, self.recv = place, left, right, send, recv
        self.sent = []

    def piece(self, d, other, p):
        pc = self.place
        core = 1 - pc.c if other else pc.c
        owner = up_to(pc.x + NX + d, NX) * 2 + core
        if p < 2:
            return self.right.at[pl.ds(2 * HB + owner * OWN + p * 4, 4)]
        return self.left.at[pl.ds(owner * OWN + (p - 2) * 4, 4)]

    def copy(self, route, p):
        pc = self.place
        shift = {0: 0, 1: 0, 2: 0, 3: -1, 4: 1, 5: -1 if p % 2 == 0 else 1, 6: 2}[route]
        to = {0: pc.along_x(1), 1: pc.along_x(-1), 5: pc.along_x(1 if p % 2 == 0 else -1)}.get(route)
        to = pc.partner() if to is None else to
        block = self.piece(shift, False, p)
        return remote(block, block, self.send.at[route, p], self.recv.at[route, p], to)

    def start(self, route, p):
        one = self.copy(route, p)
        one.start()
        self.sent.append(one)

    def arrived(self, route, p):
        shift, other = {
            0: (-1, False),
            1: (1, False),
            2: (0, True),
            3: (-1, True),
            4: (1, True),
            5: (2, False),
            6: (2, True),
        }[route]
        block = self.piece(shift, other, p)
        remote(
            block, block, self.send.at[route, p], self.recv.at[route, p], self.place.partner()
        ).wait_recv()

    def begin(self, p):
        for route in (0, 1, 2):
            self.start(route, p)

    def step(self, i):
        if i < 4:
            self.arrived(0, i)
            if i % 2 == 0:
                self.start(5, i)
            self.start(3, i)
            self.arrived(1, i)
            if i % 2 == 1:
                self.start(5, i)
            self.start(4, i)
        elif i < 8:
            self.arrived(5, i - 4)
            self.start(6, i - 4)

    def finish(self):
        for p in range(4):
            for route in (2, 3, 4, 6):
                self.arrived(route, p)


class Scatter:
    def __init__(self, place, source, bufs, send, recv, kept, make):
        self.make = make
        self.place, self.source, self.send, self.recv, self.kept = place, source, send, recv, kept
        self.s1, self.r1, self.s2, self.r2, self.sz, self.rz = bufs
        self.sent = []

    def own(self, zz, dy):
        yy = up_to(self.place.y + NY + dy, NY)
        start = pl.multiple_of((zz * NY + yy) * ROWS, 16)
        return self.source[:, pl.ds(start, ROWS), :]

    def zs(self, j):
        z = self.place.z
        return up_to(z + HALF - j, NZ), up_to(z + NZ - (HALF - 1 - j), NZ)

    def copy(self, kind, d, j):
        src, dst = ((self.s1, self.r1), (self.s2, self.r2), (self.sz, self.rz))[kind]
        way = 1 if d == 0 else -1
        to = self.place.along_z(way * leap(d, j)) if kind == 2 else self.place.along_y(way)
        return remote(src.at[d, j], dst.at[d, j], self.send.at[kind, d, j], self.recv.at[kind, d, j], to)

    def start(self, kind, d, j):
        one = self.copy(kind, d, j)
        one.start()
        self.sent.append(one)

    def first(self, j):
        za, zb = self.zs(j)
        self.make(za)
        self.make(zb)
        self.s1[0, j] = self.own(za, 2)
        self.start(0, 0, j)
        self.s1[1, j] = self.own(zb, 2)
        self.start(0, 1, j)

    def second(self, j):
        za, zb = self.zs(j)
        self.s2[0, j, 1] = self.own(zb, 1)
        self.s2[1, j, 0] = self.own(za, -1)
        self.copy(0, 0, j).wait_recv()
        self.s2[0, j, 0] = (self.r1[0, j].astype(F32) + self.own(za, 1).astype(F32)).astype(BF16)
        self.start(1, 0, j)
        self.copy(0, 1, j).wait_recv()
        self.s2[1, j, 1] = (self.r1[1, j].astype(F32) + self.own(zb, -1).astype(F32)).astype(BF16)
        self.start(1, 1, j)

    def third(self, j):
        za, zb = self.zs(j)
        self.copy(1, 0, j).wait_recv()
        self.copy(1, 1, j).wait_recv()
        sum_a = self.own(za, 0).astype(F32) + self.r2[0, j, 0].astype(F32) + self.r2[1, j, 0].astype(F32)
        sum_b = self.own(zb, 0).astype(F32) + self.r2[0, j, 1].astype(F32) + self.r2[1, j, 1].astype(F32)
        if j > 1:
            self.copy(2, 0, j - 2).wait_recv()
            sum_a = sum_a + self.rz[0, j - 2].astype(F32)
        self.sz[0, j] = sum_a.astype(BF16)
        self.start(2, 0, j)
        if j > 1:
            self.copy(2, 1, j - 2).wait_recv()
            sum_b = sum_b + self.rz[1, j - 2].astype(F32)
        if j < HALF - 1:
            self.sz[1, j] = sum_b.astype(BF16)
            self.start(2, 1, j)
        else:
            self.kept[...] = sum_b

    def slot(self, i):
        if i < HALF:
            self.first(i)
        if 0 <= i - LAG < HALF:
            self.second(i - LAG)
        if 0 <= i - 2 * LAG < HALF:
            self.third(i - 2 * LAG)

    def finish(self):
        for d, j in ((0, HALF - 2), (1, HALF - 2), (0, HALF - 1)):
            self.copy(2, d, j).wait_recv()
            self.kept[...] = self.kept[...] + self.rz[d, j].astype(F32)


class Pool:
    def __init__(self, place, pool, send, recv):
        self.place, self.pool, self.send, self.recv = place, pool, send, recv
        self.sent = []

    def copy(self, hop, d, received):
        way = 1 if d == 0 else -1
        back = -way * (hop + 1) if received else -way * hop
        yy = up_to(self.place.y + NY + back, NY)
        ref = self.pool.at[pl.ds(yy * CAP, CAP)] if hop == 0 else self.pool.at[yy * CAP + d]
        return remote(ref, ref, self.send.at[hop, d], self.recv.at[hop, d], self.place.along_y(way))

    def start(self, hop):
        for d in range(2):
            if hop == 1:
                self.copy(0, d, True).wait_recv()
            one = self.copy(hop, d, False)
            one.start()
            self.sent.append(one)

    def finish(self):
        for d in range(2):
            self.copy(1, d, True).wait_recv()


class Olds:
    def __init__(self, place, states, out, into, send, recv, kept):
        self.place, self.states, self.out, self.into = place, states, out, into
        self.send, self.recv, self.kept = send, recv, kept
        self.sent = []

    def copy(self, d, j):
        to = self.place.along_z(leap(d, j) if d == 0 else -leap(d, j))
        return remote(self.out.at[d, j], self.into.at[d, j], self.send.at[d, j], self.recv.at[d, j], to)

    def own(self, zz):
        start = pl.multiple_of((zz * NY + self.place.y) * ROWS, 16)
        return self.states[:, pl.ds(start, ROWS), :].astype(F32)

    def slot(self, j):
        z = self.place.z
        far = (up_to(z + HALF - j, NZ), up_to(z + NZ - (HALF - 1 - j), NZ))
        for d in range(2):
            value = self.own(far[d])
            if j > 1:
                self.copy(d, j - 2).wait_recv()
                value = value + self.into[d, j - 2].astype(F32)
            if d == 1 and j == HALF - 1:
                self.kept[...] = value
            else:
                self.out[d, j] = value.astype(BF16)
                one = self.copy(d, j)
                one.start()
                self.sent.append(one)

    def finish(self):
        for d, j in ((0, HALF - 2), (1, HALF - 2), (0, HALF - 1)):
            self.copy(d, j).wait_recv()
            self.kept[...] = self.kept[...] + self.into[d, j].astype(F32)


class Spread:
    def __init__(self, place, rows, zsend, zrecv, ysend, yrecv, give, take):
        self.place, self.rows, self.give, self.take = place, rows, give, take
        self.zsend, self.zrecv, self.ysend, self.yrecv = zsend, zrecv, ysend, yrecv
        self.sent = []

    def zq(self, q):
        z = self.place.z
        if q == 0:
            return z
        if q % 2 == 1:
            return up_to(z + NZ - 1 - (q - 1) // 2, NZ)
        return up_to(z + 1 + (q - 2) // 2, NZ)

    def at(self, zz, dy):
        return zz * NY + up_to(self.place.y + NY + dy, NY)

    def zcopy(self, what, d, j, received):
        z = self.place.z
        step = min(2, j + 1)
        back = j + 1 if received else j + 1 - step
        zz = up_to(z + NZ - back, NZ) if d == 0 else up_to(z + back, NZ)
        ref = self.rows.at[self.at(zz, 0), what]
        to = self.place.along_z(step if d == 0 else -step)
        return remote(ref, ref, self.zsend.at[what, d, j], self.zrecv.at[what, d, j], to)

    def ycopy(self, hop, d, q, received):
        way = 1 if d == 0 else -1
        dy = -way * (hop + 1) if received else -way * hop
        ref = self.rows.at[self.at(self.zq(q), dy), 0]
        if hop == 1:
            ref = ref.at[pl.ds(0, 64)] if d == 0 else ref.at[pl.ds(64, ROWS - 64)]
        to = self.place.along_y(way)
        return remote(ref, ref, self.ysend.at[hop, d, q], self.yrecv.at[hop, d, q], to)

    def start(self, one):
        one.start()
        self.sent.append(one)

    def out_y(self, q):
        self.start(self.ycopy(0, 0, q, False))
        self.start(self.ycopy(0, 1, q, False))

    def on_y(self, q):
        self.ycopy(0, 0, q, True).wait_recv()
        self.start(self.ycopy(1, 0, q, False))
        self.ycopy(0, 1, q, True).wait_recv()
        self.start(self.ycopy(1, 1, q, False))

    def done(self, q):
        self.ycopy(1, 0, q, True).wait_recv()
        self.ycopy(1, 1, q, True).wait_recv()
        zz = self.zq(q)
        for dy in range(NY):
            self.give(self.at(zz, dy))

    def hops(self, j):
        return (0, 1) if j < HALF - 1 else (0,)

    def along_z(self, what, j):
        for d in self.hops(j):
            self.zcopy(what, d, j, True).wait_recv()
            if j + 2 < HALF - d:
                self.start(self.zcopy(what, d, j + 2, False))
        return [1 + 2 * j + d for d in self.hops(j)]

    def begin(self, what):
        for j in range(2):
            for d in range(2):
                self.start(self.zcopy(what, d, j, False))

    def run(self, collect):
        self.out_y(0)
        self.take(self.at(self.place.z, 0))
        groups = [[0]]
        for j in range(HALF + 4):
            if j < HALF:
                for q in self.along_z(1, j):
                    self.take(self.at(self.zq(q), 0))
                if j == HALF - 1:
                    collect.first()
                group = self.along_z(0, j)
                for q in group:
                    self.out_y(q)
                groups.append(group)
            if j < len(groups):
                for q in groups[j]:
                    self.on_y(q)
            if j == HALF - 1:
                collect.second()
            if 0 <= j - 2 < len(groups):
                for q in groups[j - 2]:
                    self.done(q)


class Collect:
    def __init__(self, place, tiles, summed, out, into, relay, last, send, recv):
        self.place, self.tiles, self.summed = place, tiles, summed
        self.out, self.into, self.relay, self.last = out, into, relay, last
        self.send, self.recv = send, recv
        self.sent = []

    def copy(self, hop, d):
        src, dst = (
            (self.out.at[d], self.into.at[d]),
            (self.out.at[2, d], self.relay.at[d]),
            (self.relay.at[d], self.last.at[d]),
        )[hop]
        to = self.place.along_y(1 if d == 0 else -1)
        return remote(src, dst, self.send.at[hop, d], self.recv.at[hop, d], to)

    def start(self, hop, d):
        one = self.copy(hop, d)
        one.start()
        self.sent.append(one)

    def first(self):
        for n in (2, 0, 1):
            for s in range(CAP):
                k = self.tiles[n * CAP + s]
                for b in range(8):
                    self.out[n, s, b * 16 : (b + 1) * 16, :] = self.summed[k * 8 + b]
            if n == 2:
                self.start(1, 0)
                self.start(1, 1)
            else:
                self.start(0, n)

    def second(self):
        for d in range(2):
            self.copy(1, d).wait_recv()
            self.start(2, d)

    def finish(self):
        for hop in (0, 2):
            for d in range(2):
                self.copy(hop, d).wait_recv()

    def grad(self, s, b):
        block = slice(b * 16, (b + 1) * 16)
        value = self.summed[self.tiles[3 * CAP + s] * 8 + b].astype(F32)
        for other in (self.into[0, s, block, :], self.into[1, s, block, :], self.last[s, block, :]):
            value = value + other.astype(F32)
        return value


def dequantize(fscale, sscale, fcodes, scodes, smap, umap, exact, rounded):
    for a, (codes, table, scale) in enumerate(((fcodes, smap, fscale), (scodes, umap, sscale))):
        low_table = jnp.broadcast_to(table[0:1, :], (16, TB))
        high_table = jnp.broadcast_to(table[1:2, :], (16, TB))
        for s in range(CAP):
            for b in range(TB * TB // QB):
                block = slice(b * 16, (b + 1) * 16)
                code = codes[block, s, :]
                low = jnp.bitwise_and(code, TB - 1)
                value = jnp.where(
                    code < TB,
                    jnp.take_along_axis(low_table, low, axis=1, mode="promise_in_bounds"),
                    jnp.take_along_axis(high_table, low, axis=1, mode="promise_in_bounds"),
                )
                value = value * scale[s, b]
                exact[a, s, block, :] = value
                rounded[s, a, block, :] = value.astype(BF16)


def kernel(
    list_ref,
    slots_ref,
    rounded_ref,
    input_ref,
    grad_ref,
    gate_hbm,
    up_hbm,
    hgrad_hbm,
    update_ref,
    grad_out_ref,
    left,
    right,
    parts,
    states,
    pool,
    rows,
    summed,
    old_kept,
    sum_kept,
    oz,
    iz,
    p1,
    q1,
    p2,
    q2,
    pz,
    qz,
    cout,
    cinto,
    crelay,
    clast,
    gsend,
    grecv,
    osend,
    orecv,
    esend,
    erecv,
    psend,
    precv,
    zsend,
    zrecv,
    ysend,
    yrecv,
    csend,
    crecv,
    out_sem,
    load_sem,
    gate_ref,
    up_ref,
    hgrad_ref,
):
    place = Place()
    loads = [
        pltpu.make_async_copy(src, dst, load_sem.at[i])
        for i, (src, dst) in enumerate(((gate_hbm, gate_ref), (up_hbm, up_ref), (hgrad_hbm, hgrad_ref)))
    ]
    for one in loads:
        one.start()
    barrier = pltpu.get_barrier_semaphore()
    near = [place.partner()]
    for d in (1, -1):
        near += [place.along_x(d), place.along_y(d), place.along_z(d), place.along_z(2 * d)]
    for device in near:
        pl.semaphore_signal(barrier, inc=1, device_id=device, device_id_type=MESH)

    shared = Pool(place, pool, osend, orecv)
    pool[pl.ds(place.y * CAP, CAP)] = rounded_ref[...]
    pool[NY * CAP] = jnp.zeros((2, TB, TB), BF16)
    gather = Gather(place, left, right, gsend, grecv)
    for j in range(OWN):
        right[2 * HB + place.t * OWN + j] = grad_ref[:, j * TB : (j + 1) * TB]
    pl.semaphore_wait(barrier, len(near))
    shared.start(0)
    gather.begin(0)
    gather.begin(1)
    for j in range(OWN):
        left[place.t * OWN + j] = input_ref[:, j * TB : (j + 1) * TB].T
    gather.begin(2)
    gather.begin(3)

    def activations(i):
        for h in range(4 * i, 4 * i + 4):
            cols = slice(h * TB, (h + 1) * TB)
            gate = gate_ref[:, cols].astype(F32)
            up = up_ref[:, cols].astype(F32)
            grad = hgrad_ref[:, cols].astype(F32)
            sigmoid = 1.0 / (1.0 + jnp.exp(-gate))
            silu = gate * sigmoid
            left[WB + h] = (silu * up).astype(BF16).T
            right[h] = (grad * up * sigmoid * (1.0 + gate * (1.0 - sigmoid))).astype(BF16)
            right[HB + h] = (grad * silu).astype(BF16)

    def fill(k, carry):
        slot = slots_ref[k]
        near = lax.shift_right_logical(slot, 3) == place.z
        mine = jnp.where(near, jnp.bitwise_and(slot, NY * CAP - 1), NY * CAP)
        for a in range(2):
            states[a, pl.ds(pl.multiple_of(k * TB, TB), TB), :] = pool[mine, a]
        return carry

    olds = Olds(place, states, oz, iz, esend, erecv, old_kept)
    for one in loads:
        one.wait()
    activations(0)
    shared.start(1)
    activations(1)
    gather.step(0)
    shared.finish()
    lax.fori_loop(0, TILES, fill, 0)
    for i in range(HALF):
        if i < EARLY:
            olds.slot(i)
        gather.step(i + 1)
        if i + 2 < HB // 4:
            activations(i + 2)

    def find(k, found):
        slot = slots_ref[k]
        return tuple(jnp.where(slot == one, k, old) for one, old in zip(wanted, found))

    wanted = [
        (place.z * NY + up_to(place.y + NY + dy, NY)) * CAP + s for dy in (1, -1, 2, 0) for s in range(CAP)
    ]
    tiles = lax.fori_loop(0, TILES, find, (jnp.int32(TILES),) * len(wanted))
    summed[...] = jnp.zeros(summed.shape, BF16)
    gather.finish()

    def multiply(k, carry):
        width, hidden, matrix = list_ref[0, k], list_ref[1, k], list_ref[2, k]
        li = jnp.where(matrix == 2, WB + hidden, width)
        ri = jnp.where(matrix == 2, 2 * HB + width, jnp.where(matrix == 1, HB + hidden, hidden))
        tile = jnp.dot(left[li], right[ri], preferred_element_type=F32)
        parts[0, pl.ds(pl.multiple_of(k * TB, TB), TB), :] = tile.astype(BF16)
        return carry

    def products(zz):
        start = NY * ROWS * zz // TB
        lax.fori_loop(0, NY * ROWS // TB + 1, lambda i, carry: multiply(start + i, carry), 0, unroll=True)

    sums = Scatter(place, parts, (p1, q1, p2, q2, pz, qz), psend, precv, sum_kept, products)
    for i in range(HALF + 2 * LAG):
        sums.slot(i)
        if i + EARLY < HALF:
            olds.slot(i + EARLY)
    olds.finish()
    sums.finish()

    gives = []

    def give(dp):
        where = pl.ds(pl.multiple_of(dp * ROWS, 16), ROWS)
        one = pltpu.make_async_copy(rows.at[dp, 0], update_ref.at[where], out_sem.at[len(gives)])
        one.start()
        gives.append(one)

    def take(dp):
        summed[pl.ds(dp * (ROWS // 16), ROWS // 16)] = rows[dp, 1].reshape(ROWS // 16, 16, TB)

    collect = Collect(place, tiles, summed, cout, cinto, crelay, clast, csend, crecv)
    spread = Spread(place, rows, zsend, zrecv, ysend, yrecv, give, take)
    grad = sum_kept[0]
    rows[place.dp, 1] = grad.astype(BF16)
    spread.begin(1)
    first, second = moments(old_kept[0], old_kept[1], grad)
    first_hat = first / (1.0 - BETA_FIRST**STEP)
    second_hat = second / (1.0 - BETA_SECOND**STEP)
    rows[place.dp, 0] = (first_hat / (jnp.sqrt(second_hat) + EPSILON)).astype(BF16)
    spread.begin(0)
    spread.run(collect)
    collect.finish()
    for s in range(CAP):
        for b in range(8):
            grad_out_ref[s, b * 16 : (b + 1) * 16, :] = collect.grad(s, b)
    for phase in (shared, gather, olds, sums, spread, collect):
        for one in phase.sent:
            one.wait_send()
    for one in gives:
        one.wait()


def finish(
    update_hbm, grad_hbm, exact_hbm, out_ref, first_out, second_out, buffer, grad_ref, exact_ref, first_ref, second_ref,
    into, out, extra,
):
    count = into.shape[0]
    size = TILES * TB // count
    loads = [
        pltpu.make_async_copy(exact_hbm, exact_ref, extra.at[0]),
        pltpu.make_async_copy(grad_hbm, grad_ref, extra.at[1]),
    ]
    for one in loads:
        one.start()
    copies = []
    for i in range(count):
        where = pl.ds(i * size, size)
        one = pltpu.make_async_copy(update_hbm.at[where], buffer.at[where], into.at[i])
        one.start()
        copies.append((one, pltpu.make_async_copy(buffer.at[where], out_ref.at[where], out.at[i])))
    for one in loads:
        one.wait()
    for s in range(CAP):
        for b in range(8):
            block = slice(b * 16, (b + 1) * 16)
            first, second = moments(exact_ref[0, s, block, :], exact_ref[1, s, block, :], grad_ref[s, block, :])
            first_ref[block, s, :] = first
            second_ref[block, s, :] = second
            if s == 0:
                copies[b][0].wait()
                copies[b][1].start()
    stores = [
        pltpu.make_async_copy(first_ref, first_out, extra.at[2]),
        pltpu.make_async_copy(second_ref, second_out, extra.at[3]),
    ]
    for one in stores:
        one.start()
    for one, two in copies:
        two.wait()
    for one in stores:
        one.wait()


def body(
    layer_input,
    output_grad,
    gate_pre,
    up_pre,
    hidden_grad,
    tile_list,
    tile_slots,
    first_codes,
    second_codes,
    first_absmax,
    second_absmax,
    signed_map,
    unsigned_map,
):
    vmem = pl.BlockSpec(memory_space=pltpu.VMEM)
    smem = pl.BlockSpec(memory_space=pltpu.SMEM)
    anywhere = pl.BlockSpec(memory_space=pl.ANY)

    def scatter_shapes(n):
        one = [pltpu.VMEM((2, HALF, n, ROWS, TB), BF16)] * 2
        two = [pltpu.VMEM((2, HALF, 2, n, ROWS, TB), BF16)] * 2
        return one + two + one

    exact, rounded = pl.pallas_call(
        dequantize,
        out_shape=(
            jax.ShapeDtypeStruct((2, CAP, TB, TB), F32),
            jax.ShapeDtypeStruct((CAP, 2, TB, TB), BF16),
        ),
        in_specs=[smem] * 2 + [vmem] * 4,
        out_specs=[vmem] * 2,
    )(
        first_absmax[0],
        second_absmax[0],
        first_codes.reshape(CAP, TB, TB).transpose(1, 0, 2),
        second_codes.reshape(CAP, TB, TB).transpose(1, 0, 2),
        signed_map.reshape(2, TB),
        unsigned_map.reshape(2, TB),
    )
    dma = pltpu.SemaphoreType.DMA
    update, grad = pl.pallas_call(
        kernel,
        out_shape=(
            jax.ShapeDtypeStruct((TILES * TB, TB), BF16),
            jax.ShapeDtypeStruct((CAP, TB, TB), F32),
        ),
        in_specs=[smem] * 2 + [vmem] * 3 + [anywhere] * 3,
        out_specs=[anywhere, vmem],
        scratch_shapes=[
            pltpu.VMEM((WB + HB, TB, TB), BF16),
            pltpu.VMEM((WB + 2 * HB, TB, TB), BF16),
            pltpu.VMEM((1, TILES * TB, TB), BF16),
            pltpu.VMEM((2, TILES * TB, TB), BF16),
            pltpu.VMEM((NY * CAP + 1, 2, TB, TB), BF16),
            pltpu.VMEM((NY * NZ, 2, ROWS, TB), BF16),
            pltpu.VMEM(((TILES + 1) * 8, 16, TB), BF16),
            pltpu.VMEM((2, ROWS, TB), F32),
            pltpu.VMEM((1, ROWS, TB), F32),
        ]
        + [pltpu.VMEM((2, HALF, 2, ROWS, TB), BF16)] * 2
        + scatter_shapes(1)
        + [
            pltpu.VMEM((3, CAP, TB, TB), BF16),
            pltpu.VMEM((2, CAP, TB, TB), BF16),
            pltpu.VMEM((2, TB, TB), BF16),
            pltpu.VMEM((2, TB, TB), BF16),
        ]
        + [dma((7, 4))] * 2
        + [dma((2, 2))] * 2
        + [dma((2, HALF))] * 2
        + [dma((3, 2, HALF))] * 2
        + [dma((2, 2, HALF))] * 2
        + [dma((2, 2, NZ))] * 2
        + [dma((3, 2))] * 2
        + [dma((NY * NZ,)), dma((3,))]
        + [pltpu.VMEM(gate_pre.shape, BF16)] * 3,
        compiler_params=pltpu.CompilerParams(
            collective_id=0, has_side_effects=True, vmem_limit_bytes=60 * 1024 * 1024
        ),
    )(
        tile_list.T,
        tile_slots,
        rounded,
        layer_input,
        output_grad,
        gate_pre,
        up_pre,
        hidden_grad,
    )
    update, first, second = pl.pallas_call(
        finish,
        out_shape=(
            jax.ShapeDtypeStruct((TILES * TB, TB), BF16),
            jax.ShapeDtypeStruct((TB, CAP, TB), F32),
            jax.ShapeDtypeStruct((TB, CAP, TB), F32),
        ),
        in_specs=[anywhere] * 3,
        out_specs=[anywhere] * 3,
        scratch_shapes=[
            pltpu.VMEM((TILES * TB, TB), BF16),
            pltpu.VMEM((CAP, TB, TB), F32),
            pltpu.VMEM((2, CAP, TB, TB), F32),
            pltpu.VMEM((TB, CAP, TB), F32),
            pltpu.VMEM((TB, CAP, TB), F32),
            dma((8,)),
            dma((8,)),
            dma((4,)),
        ],
    )(update, grad, exact)
    return (
        update.reshape(TILES, TB, TB),
        first.transpose(1, 0, 2).reshape(1, CAP, TB * TB),
        second.transpose(1, 0, 2).reshape(1, CAP, TB * TB),
    )


def solution(mesh):
    in_specs = (
        P("dp", "tensor"),
        P("dp", "tensor"),
        P("dp", "tensor"),
        P("dp", "tensor"),
        P("dp", "tensor"),
        P("tensor", None),
        P("tensor"),
        P("tensor", "dp", None),
        P("tensor", "dp", None),
        P("tensor", "dp", None),
        P("tensor", "dp", None),
        P(),
        P(),
    )
    out_specs = (P("tensor", None, None), P("tensor", "dp", None), P("tensor", "dp", None))
    return jax.shard_map(body, mesh=mesh, in_specs=in_specs, out_specs=out_specs, check_vma=False)
```

```python
import functools

import jax
import jax.numpy as jnp
from jax import lax
from jax.experimental import pallas as pl
from jax.experimental.pallas import tpu as pltpu
from jax.sharding import PartitionSpec as P

CAP = 2
TB = 128
QB = 2048
STEP = 10
BETA_FIRST = 0.9
BETA_SECOND = 0.99
EPSILON = 1e-08

NX, NY, NZ = 4, 4, 16
TILES = 56
WB = 64
HB = 28
OWN = WB // 8
ROWS = TILES * TB // (NY * NZ)
HALF = NZ // 2
LAG = 2
EARLY = 4
MESH = pl.DeviceIdType.MESH
F32, BF16 = jnp.float32, jnp.bfloat16


def up_to(value, size):
    return lax.rem(value, size)


class Place:
    def __init__(self):
        dp, t = lax.axis_index("dp"), lax.axis_index("tensor")
        self.dp, self.t = dp, t
        self.z, self.y = dp // NY, lax.rem(dp, NY)
        self.x, self.c = t // 2, lax.rem(t, 2)

    def along_x(self, d):
        return (self.dp, up_to(self.x + NX + d, NX) * 2 + self.c)

    def partner(self):
        return (self.dp, self.x * 2 + 1 - self.c)

    def along_y(self, d):
        return (self.z * NY + up_to(self.y + NY + d, NY), self.t)

    def along_z(self, d):
        return (up_to(self.z + NZ + d, NZ) * NY + self.y, self.t)


def remote(src, dst, send, recv, device):
    return pltpu.make_async_remote_copy(
        src_ref=src, dst_ref=dst, send_sem=send, recv_sem=recv, device_id=device, device_id_type=MESH
    )


def moments(first_old, second_old, grad):
    first = BETA_FIRST * first_old + (1.0 - BETA_FIRST) * grad
    second = BETA_SECOND * second_old + (1.0 - BETA_SECOND) * grad * grad
    return first, second


def leap(d, j):
    return min(2, HALF - d - j)


class Gather:
    def __init__(self, place, left, right, send, recv):
        self.place, self.left, self.right, self.send, self.recv = place, left, right, send, recv
        self.sent = []

    def piece(self, d, other, p):
        pc = self.place
        core = 1 - pc.c if other else pc.c
        owner = up_to(pc.x + NX + d, NX) * 2 + core
        if p < 2:
            return self.right.at[pl.ds(2 * HB + owner * OWN + p * 4, 4)]
        return self.left.at[pl.ds(owner * OWN + (p - 2) * 4, 4)]

    def copy(self, route, p):
        pc = self.place
        shift = {0: 0, 1: 0, 2: 0, 3: -1, 4: 1, 5: -1 if p % 2 == 0 else 1, 6: 2}[route]
        to = {0: pc.along_x(1), 1: pc.along_x(-1), 5: pc.along_x(1 if p % 2 == 0 else -1)}.get(route)
        to = pc.partner() if to is None else to
        block = self.piece(shift, False, p)
        return remote(block, block, self.send.at[route, p], self.recv.at[route, p], to)

    def start(self, route, p):
        one = self.copy(route, p)
        one.start()
        self.sent.append(one)

    def arrived(self, route, p):
        shift, other = {
            0: (-1, False),
            1: (1, False),
            2: (0, True),
            3: (-1, True),
            4: (1, True),
            5: (2, False),
            6: (2, True),
        }[route]
        block = self.piece(shift, other, p)
        remote(
            block, block, self.send.at[route, p], self.recv.at[route, p], self.place.partner()
        ).wait_recv()

    def begin(self, p):
        for route in (0, 1, 2):
            self.start(route, p)

    def step(self, i):
        if i < 4:
            self.arrived(0, i)
            if i % 2 == 0:
                self.start(5, i)
            self.start(3, i)
            self.arrived(1, i)
            if i % 2 == 1:
                self.start(5, i)
            self.start(4, i)
        elif i < 8:
            self.arrived(5, i - 4)
            self.start(6, i - 4)

    def finish(self):
        for p in range(4):
            for route in (2, 3, 4, 6):
                self.arrived(route, p)


class Scatter:
    def __init__(self, place, source, bufs, send, recv, kept, make):
        self.make = make
        self.place, self.source, self.send, self.recv, self.kept = place, source, send, recv, kept
        self.s1, self.r1, self.s2, self.r2, self.sz, self.rz = bufs
        self.sent = []

    def own(self, zz, dy):
        yy = up_to(self.place.y + NY + dy, NY)
        start = pl.multiple_of((zz * NY + yy) * ROWS, 16)
        return self.source[:, pl.ds(start, ROWS), :]

    def zs(self, j):
        z = self.place.z
        return up_to(z + HALF - j, NZ), up_to(z + NZ - (HALF - 1 - j), NZ)

    def copy(self, kind, d, j):
        src, dst = ((self.s1, self.r1), (self.s2, self.r2), (self.sz, self.rz))[kind]
        way = 1 if d == 0 else -1
        to = self.place.along_z(way * leap(d, j)) if kind == 2 else self.place.along_y(way)
        return remote(src.at[d, j], dst.at[d, j], self.send.at[kind, d, j], self.recv.at[kind, d, j], to)

    def start(self, kind, d, j):
        one = self.copy(kind, d, j)
        one.start()
        self.sent.append(one)

    def first(self, j):
        za, zb = self.zs(j)
        self.make(za)
        self.make(zb)
        self.s1[0, j] = self.own(za, 2)
        self.start(0, 0, j)
        self.s1[1, j] = self.own(zb, 2)
        self.start(0, 1, j)

    def second(self, j):
        za, zb = self.zs(j)
        self.s2[0, j, 1] = self.own(zb, 1)
        self.s2[1, j, 0] = self.own(za, -1)
        self.copy(0, 0, j).wait_recv()
        self.s2[0, j, 0] = (self.r1[0, j].astype(F32) + self.own(za, 1).astype(F32)).astype(BF16)
        self.start(1, 0, j)
        self.copy(0, 1, j).wait_recv()
        self.s2[1, j, 1] = (self.r1[1, j].astype(F32) + self.own(zb, -1).astype(F32)).astype(BF16)
        self.start(1, 1, j)

    def third(self, j):
        za, zb = self.zs(j)
        self.copy(1, 0, j).wait_recv()
        self.copy(1, 1, j).wait_recv()
        sum_a = self.own(za, 0).astype(F32) + self.r2[0, j, 0].astype(F32) + self.r2[1, j, 0].astype(F32)
        sum_b = self.own(zb, 0).astype(F32) + self.r2[0, j, 1].astype(F32) + self.r2[1, j, 1].astype(F32)
        if j > 1:
            self.copy(2, 0, j - 2).wait_recv()
            sum_a = sum_a + self.rz[0, j - 2].astype(F32)
        self.sz[0, j] = sum_a.astype(BF16)
        self.start(2, 0, j)
        if j > 1:
            self.copy(2, 1, j - 2).wait_recv()
            sum_b = sum_b + self.rz[1, j - 2].astype(F32)
        if j < HALF - 1:
            self.sz[1, j] = sum_b.astype(BF16)
            self.start(2, 1, j)
        else:
            self.kept[...] = sum_b

    def slot(self, i):
        if i < HALF:
            self.first(i)
        if 0 <= i - LAG < HALF:
            self.second(i - LAG)
        if 0 <= i - 2 * LAG < HALF:
            self.third(i - 2 * LAG)

    def finish(self):
        for d, j in ((0, HALF - 2), (1, HALF - 2), (0, HALF - 1)):
            self.copy(2, d, j).wait_recv()
            self.kept[...] = self.kept[...] + self.rz[d, j].astype(F32)


class Pool:
    def __init__(self, place, pool, send, recv):
        self.place, self.pool, self.send, self.recv = place, pool, send, recv
        self.sent = []

    def copy(self, hop, d, received):
        way = 1 if d == 0 else -1
        back = -way * (hop + 1) if received else -way * hop
        yy = up_to(self.place.y + NY + back, NY)
        ref = self.pool.at[pl.ds(yy * CAP, CAP)] if hop == 0 else self.pool.at[yy * CAP + d]
        return remote(ref, ref, self.send.at[hop, d], self.recv.at[hop, d], self.place.along_y(way))

    def start(self, hop):
        for d in range(2):
            if hop == 1:
                self.copy(0, d, True).wait_recv()
            one = self.copy(hop, d, False)
            one.start()
            self.sent.append(one)

    def finish(self):
        for d in range(2):
            self.copy(1, d, True).wait_recv()


class Olds:
    def __init__(self, place, states, out, into, send, recv, kept):
        self.place, self.states, self.out, self.into = place, states, out, into
        self.send, self.recv, self.kept = send, recv, kept
        self.sent = []

    def copy(self, d, j):
        to = self.place.along_z(leap(d, j) if d == 0 else -leap(d, j))
        return remote(self.out.at[d, j], self.into.at[d, j], self.send.at[d, j], self.recv.at[d, j], to)

    def own(self, zz):
        start = pl.multiple_of((zz * NY + self.place.y) * ROWS, 16)
        return self.states[:, pl.ds(start, ROWS), :].astype(F32)

    def slot(self, j):
        z = self.place.z
        far = (up_to(z + HALF - j, NZ), up_to(z + NZ - (HALF - 1 - j), NZ))
        for d in range(2):
            value = self.own(far[d])
            if j > 1:
                self.copy(d, j - 2).wait_recv()
                value = value + self.into[d, j - 2].astype(F32)
            if d == 1 and j == HALF - 1:
                self.kept[...] = value
            else:
                self.out[d, j] = value.astype(BF16)
                one = self.copy(d, j)
                one.start()
                self.sent.append(one)

    def finish(self):
        for d, j in ((0, HALF - 2), (1, HALF - 2), (0, HALF - 1)):
            self.copy(d, j).wait_recv()
            self.kept[...] = self.kept[...] + self.into[d, j].astype(F32)


class Spread:
    def __init__(self, place, rows, zsend, zrecv, ysend, yrecv, give, take):
        self.place, self.rows, self.give, self.take = place, rows, give, take
        self.zsend, self.zrecv, self.ysend, self.yrecv = zsend, zrecv, ysend, yrecv
        self.sent = []

    def zq(self, q):
        z = self.place.z
        if q == 0:
            return z
        if q % 2 == 1:
            return up_to(z + NZ - 1 - (q - 1) // 2, NZ)
        return up_to(z + 1 + (q - 2) // 2, NZ)

    def at(self, zz, dy):
        return zz * NY + up_to(self.place.y + NY + dy, NY)

    def zcopy(self, what, d, j, received):
        z = self.place.z
        step = min(2, j + 1)
        back = j + 1 if received else j + 1 - step
        zz = up_to(z + NZ - back, NZ) if d == 0 else up_to(z + back, NZ)
        ref = self.rows.at[self.at(zz, 0), what]
        to = self.place.along_z(step if d == 0 else -step)
        return remote(ref, ref, self.zsend.at[what, d, j], self.zrecv.at[what, d, j], to)

    def ycopy(self, hop, d, q, received):
        way = 1 if d == 0 else -1
        dy = -way * (hop + 1) if received else -way * hop
        ref = self.rows.at[self.at(self.zq(q), dy), 0]
        if hop == 1:
            ref = ref.at[pl.ds(0, 64)] if d == 0 else ref.at[pl.ds(64, ROWS - 64)]
        to = self.place.along_y(way)
        return remote(ref, ref, self.ysend.at[hop, d, q], self.yrecv.at[hop, d, q], to)

    def start(self, one):
        one.start()
        self.sent.append(one)

    def out_y(self, q):
        self.start(self.ycopy(0, 0, q, False))
        self.start(self.ycopy(0, 1, q, False))

    def on_y(self, q):
        self.ycopy(0, 0, q, True).wait_recv()
        self.start(self.ycopy(1, 0, q, False))
        self.ycopy(0, 1, q, True).wait_recv()
        self.start(self.ycopy(1, 1, q, False))

    def done(self, q):
        self.ycopy(1, 0, q, True).wait_recv()
        self.ycopy(1, 1, q, True).wait_recv()
        zz = self.zq(q)
        for dy in range(NY):
            self.give(self.at(zz, dy))

    def hops(self, j):
        return (0, 1) if j < HALF - 1 else (0,)

    def along_z(self, what, j):
        for d in self.hops(j):
            self.zcopy(what, d, j, True).wait_recv()
            if j + 2 < HALF - d:
                self.start(self.zcopy(what, d, j + 2, False))
        return [1 + 2 * j + d for d in self.hops(j)]

    def begin(self, what):
        for j in range(2):
            for d in range(2):
                self.start(self.zcopy(what, d, j, False))

    def run(self, collect):
        self.out_y(0)
        self.take(self.at(self.place.z, 0))
        groups = [[0]]
        for j in range(HALF + 4):
            if j < HALF:
                for q in self.along_z(1, j):
                    self.take(self.at(self.zq(q), 0))
                if j == HALF - 1:
                    collect.first()
                group = self.along_z(0, j)
                for q in group:
                    self.out_y(q)
                groups.append(group)
            if j == HALF:
                collect.second()
            if 0 <= j - 1 < len(groups):
                for q in groups[j - 1]:
                    self.on_y(q)
            if 0 <= j - 3 < len(groups):
                for q in groups[j - 3]:
                    self.done(q)


class Collect:
    def __init__(self, place, tiles, summed, out, into, relay, last, send, recv):
        self.place, self.tiles, self.summed = place, tiles, summed
        self.out, self.into, self.relay, self.last = out, into, relay, last
        self.send, self.recv = send, recv
        self.sent = []

    def copy(self, hop, d):
        src, dst = (
            (self.out.at[d], self.into.at[d]),
            (self.out.at[2, d], self.relay.at[d]),
            (self.relay.at[d], self.last.at[d]),
        )[hop]
        to = self.place.along_y(1 if d == 0 else -1)
        return remote(src, dst, self.send.at[hop, d], self.recv.at[hop, d], to)

    def start(self, hop, d):
        one = self.copy(hop, d)
        one.start()
        self.sent.append(one)

    def first(self):
        for n in (2, 0, 1):
            for s in range(CAP):
                k = self.tiles[n * CAP + s]
                for b in range(8):
                    self.out[n, s, b * 16 : (b + 1) * 16, :] = self.summed[k * 8 + b]
            if n == 2:
                self.start(1, 0)
                self.start(1, 1)
            else:
                self.start(0, n)

    def second(self):
        for d in range(2):
            self.copy(1, d).wait_recv()
            self.start(2, d)

    def finish(self):
        for hop in (0, 2):
            for d in range(2):
                self.copy(hop, d).wait_recv()

    def grad(self, s, b):
        block = slice(b * 16, (b + 1) * 16)
        value = self.summed[self.tiles[3 * CAP + s] * 8 + b].astype(F32)
        for other in (self.into[0, s, block, :], self.into[1, s, block, :], self.last[s, block, :]):
            value = value + other.astype(F32)
        return value


def dequantize(fscale, sscale, fcodes, scodes, smap, umap, exact, rounded):
    for a, (codes, table, scale) in enumerate(((fcodes, smap, fscale), (scodes, umap, sscale))):
        low_table = jnp.broadcast_to(table[0:1, :], (16, TB))
        high_table = jnp.broadcast_to(table[1:2, :], (16, TB))
        for s in range(CAP):
            for b in range(TB * TB // QB):
                block = slice(b * 16, (b + 1) * 16)
                code = codes[block, s, :]
                low = jnp.bitwise_and(code, TB - 1)
                value = jnp.where(
                    code < TB,
                    jnp.take_along_axis(low_table, low, axis=1, mode="promise_in_bounds"),
                    jnp.take_along_axis(high_table, low, axis=1, mode="promise_in_bounds"),
                )
                value = value * scale[s, b]
                exact[a, s, block, :] = value
                rounded[s, a, block, :] = value.astype(BF16)


def kernel(
    list_ref,
    slots_ref,
    rounded_ref,
    input_ref,
    grad_ref,
    gate_hbm,
    up_hbm,
    hgrad_hbm,
    update_ref,
    grad_out_ref,
    left,
    right,
    parts,
    states,
    pool,
    rows,
    summed,
    old_kept,
    sum_kept,
    oz,
    iz,
    p1,
    q1,
    p2,
    q2,
    pz,
    qz,
    cout,
    cinto,
    crelay,
    clast,
    gsend,
    grecv,
    osend,
    orecv,
    esend,
    erecv,
    psend,
    precv,
    zsend,
    zrecv,
    ysend,
    yrecv,
    csend,
    crecv,
    out_sem,
    load_sem,
    gate_ref,
    up_ref,
    hgrad_ref,
):
    place = Place()
    loads = [
        pltpu.make_async_copy(src, dst, load_sem.at[i])
        for i, (src, dst) in enumerate(((gate_hbm, gate_ref), (up_hbm, up_ref), (hgrad_hbm, hgrad_ref)))
    ]
    for one in loads:
        one.start()
    barrier = pltpu.get_barrier_semaphore()
    near = [place.partner()]
    for d in (1, -1):
        near += [place.along_x(d), place.along_y(d), place.along_z(d), place.along_z(2 * d)]
    for device in near:
        pl.semaphore_signal(barrier, inc=1, device_id=device, device_id_type=MESH)

    shared = Pool(place, pool, osend, orecv)
    pool[pl.ds(place.y * CAP, CAP)] = rounded_ref[...]
    pool[NY * CAP] = jnp.zeros((2, TB, TB), BF16)
    gather = Gather(place, left, right, gsend, grecv)
    for j in range(OWN):
        right[2 * HB + place.t * OWN + j] = grad_ref[:, j * TB : (j + 1) * TB]
    pl.semaphore_wait(barrier, len(near))
    shared.start(0)
    gather.begin(0)
    gather.begin(1)
    for j in range(OWN):
        left[place.t * OWN + j] = input_ref[:, j * TB : (j + 1) * TB].T
    gather.begin(2)
    gather.begin(3)

    def activations(i):
        for h in range(4 * i, 4 * i + 4):
            cols = slice(h * TB, (h + 1) * TB)
            gate = gate_ref[:, cols].astype(F32)
            up = up_ref[:, cols].astype(F32)
            grad = hgrad_ref[:, cols].astype(F32)
            sigmoid = 1.0 / (1.0 + jnp.exp(-gate))
            silu = gate * sigmoid
            left[WB + h] = (silu * up).astype(BF16).T
            right[h] = (grad * up * sigmoid * (1.0 + gate * (1.0 - sigmoid))).astype(BF16)
            right[HB + h] = (grad * silu).astype(BF16)

    def fill(k, carry):
        slot = slots_ref[k]
        near = lax.shift_right_logical(slot, 3) == place.z
        mine = jnp.where(near, jnp.bitwise_and(slot, NY * CAP - 1), NY * CAP)
        for a in range(2):
            states[a, pl.ds(pl.multiple_of(k * TB, TB), TB), :] = pool[mine, a]
        return carry

    olds = Olds(place, states, oz, iz, esend, erecv, old_kept)
    for one in loads:
        one.wait()
    activations(0)
    shared.start(1)
    activations(1)
    gather.step(0)
    shared.finish()
    lax.fori_loop(0, TILES, fill, 0)
    for i in range(HALF):
        if i < EARLY:
            olds.slot(i)
        gather.step(i + 1)
        if i + 2 < HB // 4:
            activations(i + 2)

    def find(k, found):
        slot = slots_ref[k]
        return tuple(jnp.where(slot == one, k, old) for one, old in zip(wanted, found))

    wanted = [
        (place.z * NY + up_to(place.y + NY + dy, NY)) * CAP + s for dy in (1, -1, 2, 0) for s in range(CAP)
    ]
    tiles = lax.fori_loop(0, TILES, find, (jnp.int32(TILES),) * len(wanted))
    summed[...] = jnp.zeros(summed.shape, BF16)
    gather.finish()

    def multiply(k, carry):
        width, hidden, matrix = list_ref[0, k], list_ref[1, k], list_ref[2, k]
        li = jnp.where(matrix == 2, WB + hidden, width)
        ri = jnp.where(matrix == 2, 2 * HB + width, jnp.where(matrix == 1, HB + hidden, hidden))
        tile = jnp.dot(left[li], right[ri], preferred_element_type=F32)
        parts[0, pl.ds(pl.multiple_of(k * TB, TB), TB), :] = tile.astype(BF16)
        return carry

    def products(zz):
        start = NY * ROWS * zz // TB
        lax.fori_loop(0, NY * ROWS // TB + 1, lambda i, carry: multiply(start + i, carry), 0, unroll=True)

    sums = Scatter(place, parts, (p1, q1, p2, q2, pz, qz), psend, precv, sum_kept, products)
    for i in range(HALF + 2 * LAG):
        sums.slot(i)
        if i + EARLY < HALF:
            olds.slot(i + EARLY)
    olds.finish()
    sums.finish()

    gives = []

    def give(dp):
        where = pl.ds(pl.multiple_of(dp * ROWS, 16), ROWS)
        one = pltpu.make_async_copy(rows.at[dp, 0], update_ref.at[where], out_sem.at[len(gives)])
        one.start()
        gives.append(one)

    def take(dp):
        summed[pl.ds(dp * (ROWS // 16), ROWS // 16)] = rows[dp, 1].reshape(ROWS // 16, 16, TB)

    collect = Collect(place, tiles, summed, cout, cinto, crelay, clast, csend, crecv)
    spread = Spread(place, rows, zsend, zrecv, ysend, yrecv, give, take)
    grad = sum_kept[0]
    rows[place.dp, 1] = grad.astype(BF16)
    spread.begin(1)
    first, second = moments(old_kept[0], old_kept[1], grad)
    first_hat = first / (1.0 - BETA_FIRST**STEP)
    second_hat = second / (1.0 - BETA_SECOND**STEP)
    rows[place.dp, 0] = (first_hat / (jnp.sqrt(second_hat) + EPSILON)).astype(BF16)
    spread.begin(0)
    spread.run(collect)
    collect.finish()
    for s in range(CAP):
        for b in range(8):
            grad_out_ref[s, b * 16 : (b + 1) * 16, :] = collect.grad(s, b)
    for phase in (shared, gather, olds, sums, spread, collect):
        for one in phase.sent:
            one.wait_send()
    for one in gives:
        one.wait()


def finish(
    update_hbm, grad_hbm, exact_hbm, out_ref, first_out, second_out, buffer, grad_ref, exact_ref, first_ref, second_ref,
    into, out, extra,
):
    count = into.shape[0]
    size = TILES * TB // count
    loads = [
        pltpu.make_async_copy(exact_hbm, exact_ref, extra.at[0]),
        pltpu.make_async_copy(grad_hbm, grad_ref, extra.at[1]),
    ]
    for one in loads:
        one.start()
    copies = []
    for i in range(count):
        where = pl.ds(i * size, size)
        one = pltpu.make_async_copy(update_hbm.at[where], buffer.at[where], into.at[i])
        one.start()
        copies.append((one, pltpu.make_async_copy(buffer.at[where], out_ref.at[where], out.at[i])))
    for one in loads:
        one.wait()
    for s in range(CAP):
        for b in range(8):
            block = slice(b * 16, (b + 1) * 16)
            first, second = moments(exact_ref[0, s, block, :], exact_ref[1, s, block, :], grad_ref[s, block, :])
            first_ref[block, s, :] = first
            second_ref[block, s, :] = second
            if s == 0:
                copies[b][0].wait()
                copies[b][1].start()
    stores = [
        pltpu.make_async_copy(first_ref, first_out, extra.at[2]),
        pltpu.make_async_copy(second_ref, second_out, extra.at[3]),
    ]
    for one in stores:
        one.start()
    for one, two in copies:
        two.wait()
    for one in stores:
        one.wait()


def body(
    layer_input,
    output_grad,
    gate_pre,
    up_pre,
    hidden_grad,
    tile_list,
    tile_slots,
    first_codes,
    second_codes,
    first_absmax,
    second_absmax,
    signed_map,
    unsigned_map,
):
    vmem = pl.BlockSpec(memory_space=pltpu.VMEM)
    smem = pl.BlockSpec(memory_space=pltpu.SMEM)
    anywhere = pl.BlockSpec(memory_space=pl.ANY)

    def scatter_shapes(n):
        one = [pltpu.VMEM((2, HALF, n, ROWS, TB), BF16)] * 2
        two = [pltpu.VMEM((2, HALF, 2, n, ROWS, TB), BF16)] * 2
        return one + two + one

    exact, rounded = pl.pallas_call(
        dequantize,
        out_shape=(
            jax.ShapeDtypeStruct((2, CAP, TB, TB), F32),
            jax.ShapeDtypeStruct((CAP, 2, TB, TB), BF16),
        ),
        in_specs=[smem] * 2 + [vmem] * 4,
        out_specs=[vmem] * 2,
    )(
        first_absmax[0],
        second_absmax[0],
        first_codes.reshape(CAP, TB, TB).transpose(1, 0, 2),
        second_codes.reshape(CAP, TB, TB).transpose(1, 0, 2),
        signed_map.reshape(2, TB),
        unsigned_map.reshape(2, TB),
    )
    dma = pltpu.SemaphoreType.DMA
    update, grad = pl.pallas_call(
        kernel,
        out_shape=(
            jax.ShapeDtypeStruct((TILES * TB, TB), BF16),
            jax.ShapeDtypeStruct((CAP, TB, TB), F32),
        ),
        in_specs=[smem] * 2 + [vmem] * 3 + [anywhere] * 3,
        out_specs=[anywhere, vmem],
        scratch_shapes=[
            pltpu.VMEM((WB + HB, TB, TB), BF16),
            pltpu.VMEM((WB + 2 * HB, TB, TB), BF16),
            pltpu.VMEM((1, TILES * TB, TB), BF16),
            pltpu.VMEM((2, TILES * TB, TB), BF16),
            pltpu.VMEM((NY * CAP + 1, 2, TB, TB), BF16),
            pltpu.VMEM((NY * NZ, 2, ROWS, TB), BF16),
            pltpu.VMEM(((TILES + 1) * 8, 16, TB), BF16),
            pltpu.VMEM((2, ROWS, TB), F32),
            pltpu.VMEM((1, ROWS, TB), F32),
        ]
        + [pltpu.VMEM((2, HALF, 2, ROWS, TB), BF16)] * 2
        + scatter_shapes(1)
        + [
            pltpu.VMEM((3, CAP, TB, TB), BF16),
            pltpu.VMEM((2, CAP, TB, TB), BF16),
            pltpu.VMEM((2, TB, TB), BF16),
            pltpu.VMEM((2, TB, TB), BF16),
        ]
        + [dma((7, 4))] * 2
        + [dma((2, 2))] * 2
        + [dma((2, HALF))] * 2
        + [dma((3, 2, HALF))] * 2
        + [dma((2, 2, HALF))] * 2
        + [dma((2, 2, NZ))] * 2
        + [dma((3, 2))] * 2
        + [dma((NY * NZ,)), dma((3,))]
        + [pltpu.VMEM(gate_pre.shape, BF16)] * 3,
        compiler_params=pltpu.CompilerParams(
            collective_id=0, has_side_effects=True, vmem_limit_bytes=60 * 1024 * 1024
        ),
    )(
        tile_list.T,
        tile_slots,
        rounded,
        layer_input,
        output_grad,
        gate_pre,
        up_pre,
        hidden_grad,
    )
    update, first, second = pl.pallas_call(
        finish,
        out_shape=(
            jax.ShapeDtypeStruct((TILES * TB, TB), BF16),
            jax.ShapeDtypeStruct((TB, CAP, TB), F32),
            jax.ShapeDtypeStruct((TB, CAP, TB), F32),
        ),
        in_specs=[anywhere] * 3,
        out_specs=[anywhere] * 3,
        scratch_shapes=[
            pltpu.VMEM((TILES * TB, TB), BF16),
            pltpu.VMEM((CAP, TB, TB), F32),
            pltpu.VMEM((2, CAP, TB, TB), F32),
            pltpu.VMEM((TB, CAP, TB), F32),
            pltpu.VMEM((TB, CAP, TB), F32),
            dma((8,)),
            dma((8,)),
            dma((4,)),
        ],
    )(update, grad, exact)
    return (
        update.reshape(TILES, TB, TB),
        first.transpose(1, 0, 2).reshape(1, CAP, TB * TB),
        second.transpose(1, 0, 2).reshape(1, CAP, TB * TB),
    )


def solution(mesh):
    in_specs = (
        P("dp", "tensor"),
        P("dp", "tensor"),
        P("dp", "tensor"),
        P("dp", "tensor"),
        P("dp", "tensor"),
        P("tensor", None),
        P("tensor"),
        P("tensor", "dp", None),
        P("tensor", "dp", None),
        P("tensor", "dp", None),
        P("tensor", "dp", None),
        P(),
        P(),
    )
    out_specs = (P("tensor", None, None), P("tensor", "dp", None), P("tensor", "dp", None))
    return jax.shard_map(body, mesh=mesh, in_specs=in_specs, out_specs=out_specs, check_vma=False)
```
